32 devices in a mesh: groups: 2 (over y), expert: 8 (over z, core), dp: 2 (over x).
Axes of the slice: x: 2, y: 2, z: 4, core: 2. Of those that a mesh axis runs over, the one named last changes fastest.
Arguments:
- tokens: bfloat16 [1024, 2048], P(('groups', 'expert'), 'dp'), parts along dimension 0, may hold values from -6 to 6
- expert_ids: int32 [1024, 8], P(('groups', 'expert')), parts along dimension 0, may hold values from 0 to 15, all different within a row; in each aligned block of 64 rows (0 to 63, 64 to 127, ...) at most 64 rows name the same one
- gate_levels: int32 [1024, 8], P(('groups', 'expert')), parts along dimension 0, may hold values from 1 to 255
- gate_weight: bfloat16 [16, 2048, 1536], P('expert', None, 'dp'), may hold values from -0.125 to 0.125
- up_weight: bfloat16 [16, 2048, 1536], P('expert', None, 'dp'), may hold values from -0.125 to 0.125
- down_weight: bfloat16 [16, 1536, 2048], P('expert', None, 'dp'), may hold values from -0.15625 to 0.15625
Outputs:
- mixed: bfloat16 [1024, 2048], P(('groups', 'expert'), 'dp'), parts along dimension 0
The draws below stay inside these ranges and needn't reach their ends.
There are 2 independent parts, one for each index of `groups`. The reference program is written for one: setup_inputs(seed, part) draws one part's arguments, and reference() takes and returns one part's arrays. A program takes and returns all parts, laid end to end along the dimension named above; an argument that names none is the same for every part. Nothing has to cross between parts.
Inputs may be any that keep to these rules, and one draw needn't show every extreme that they name: `expert_ids`: each row names 8 different experts. Among the rows of one index of the expert axis no expert is named more than 64 times, a bound that some block reaches.
All inputs are finite; a program needn't handle non-finite values.
Results may differ from the reference program's by a relative error of at most 0.0057.
Values may be sent and summed in bfloat16 or wider, within the bound.
A program may use at most 64 MiB of HBM per device.

```python
import math
import jax
import jax.numpy as jnp
import numpy as np
from jax import lax

D = 2048
FF = 1536
TOP = 8
TOK_DEV = 64
EXPERTS = 16
TOKENS = 512
CAP = 64
N_EXPERT = 8


def with_ends(drawn, key, least, top_value):
    longest = drawn.shape.index(max(drawn.shape))
    spots = []
    for shift in (0, 1):
        where = [jax.random.randint(jax.random.fold_in(key, axis), (), 0, length) for axis, length in enumerate(drawn.shape)]
        where[longest] = (where[longest] + shift) % drawn.shape[longest]
        spots.append(tuple(where))
    return drawn.at[spots[0]].set(least).at[spots[1]].set(top_value)


def level_of(own_key, dims, split, least, largest):
    def one(dim, blocks):
        steps = jax.random.uniform(jax.random.fold_in(jax.random.fold_in(own_key, 6), dim), (blocks,), jnp.float32, least / len(split), largest / len(split))
        return jnp.repeat(jnp.exp(steps), dims[dim] // blocks).reshape((-1,) + (1,) * (len(dims) - dim - 1))

    level = one(*split[0])
    for cut in split[1:]:
        level = level * one(*cut)
    return level


def routed_block(key, own, number, rows, number_of, top, bound, skew):
    ranking = jax.random.permutation(key, number_of)
    packed, usual = load_shares(number_of, rows * top, bound, skew, True), load_shares(number_of, rows * top, bound, skew, False)
    places = jnp.arange(number_of)

    def named(lengths, turn):
        used = int((lengths > 0).sum())
        fixed = max(1, used // 4)
        shifted = fixed + (places - fixed + turn * (used - fixed)) % max(1, number_of - fixed)
        return jnp.zeros((number_of,), jnp.int32).at[ranking[jnp.where(places < fixed, places, shifted)]].set(jnp.asarray(lengths, jnp.int32))

    lengths = jnp.where(number % 4 == 0, named(packed, number // 4), named(usual, number - number // 4 - 1))
    mixed = jax.random.permutation(jax.random.fold_in(own, 3), number_of)
    donor, sink = mixed[0:number_of // 2 * 2:2], mixed[1:number_of // 2 * 2:2]
    slack = jnp.minimum(lengths[donor] - 1, bound - lengths[sink]) // 2
    slack = jnp.where((donor == ranking[0]) | (sink == ranking[0]) | (lengths[sink] == 0), 0, jnp.maximum(slack, 0))
    shifted = jax.random.randint(jax.random.fold_in(own, 4), (number_of // 2,), 0, 1 << 20) % (slack + 1)
    lengths = lengths.at[donor].add(-shifted).at[sink].add(shifted)
    members = jnp.searchsorted(jnp.cumsum(lengths), jnp.arange(rows * top), side="right").astype(jnp.int32)
    grid = members.reshape(top, rows).T
    grid = grid[jax.random.permutation(jax.random.fold_in(own, 1), rows)]
    turn = jax.random.randint(jax.random.fold_in(own, 2), (rows, 1), 0, top)
    return jnp.take_along_axis(grid, (jnp.arange(top)[None, :] + turn) % top, axis=1)


def load_shares(amount, total, most, lean, full):
    weights = [(1 << 20) // math.isqrt(grade ** lean) + 1 for grade in range(1, amount + 1)]
    largest = most if full else min(most, max(-(-total // amount), total * weights[0] // sum(weights)))
    least = 1 if total - largest >= amount - 1 else 0
    given, rest = [largest] + [least] * (amount - 1), total - largest - least * (amount - 1)
    while rest > 0:
        candidates = [i for i in range(1, amount) if given[i] < largest] or [i for i in range(1, amount) if given[i] < most]
        mass, budget = sum([weights[i] for i in candidates]), rest
        for i in candidates:
            extra = min(most - given[i], max(1, budget * weights[i] // mass), rest)
            given[i] = given[i] + extra
            rest = rest - extra
    return np.array(given)


def bell_draw(key, shape, scale, reach, split=(), kind=jnp.bfloat16):
    array = jax.random.normal(key, shape, jnp.float32) * scale
    if len(split) > 0:
        array = level_of(key, shape, split, -0.22, 0.18) * array
    return jnp.clip(array, min=-reach, max=reach).astype(kind)


def setup_inputs(seed: int = 0, part: int = 0) -> dict:
    arg_keys = jax.random.split(jax.random.key(seed), 7)
    own_keys = jax.random.split(jax.random.fold_in(arg_keys[6], part), 7)
    tokens = bell_draw(own_keys[0], (TOKENS, D), 1.0, 6.0, ((0, 8), (1, 2)))
    expert_ids_keys = jax.random.split(jax.random.fold_in(own_keys[1], 1), TOKENS // TOK_DEV)
    expert_ids_turns = jax.random.permutation(jax.random.fold_in(own_keys[1], 3), TOKENS // TOK_DEV)
    expert_ids = jax.vmap(lambda own, number: routed_block(jax.random.fold_in(own_keys[1], 2), own, number, TOK_DEV, EXPERTS, TOP, CAP, 2))(expert_ids_keys, expert_ids_turns).reshape((TOKENS, TOP))
    gate_levels = with_ends(jax.random.randint(own_keys[2], (TOKENS, TOP), 1, 256), jax.random.fold_in(own_keys[2], 1), 1, 255).astype(jnp.int32)
    gate_weight = bell_draw(arg_keys[3], (EXPERTS, D, FF), D ** -0.5, 0.125, ((0, 8), (2, 2)))
    up_weight = bell_draw(arg_keys[4], (EXPERTS, D, FF), D ** -0.5, 0.125, ((0, 8), (2, 2)))
    down_weight = bell_draw(arg_keys[5], (EXPERTS, FF, D), FF ** -0.5, 0.15625, ((0, 8), (2, 2)))
    return dict(tokens=tokens, expert_ids=expert_ids, gate_levels=gate_levels, gate_weight=gate_weight, up_weight=up_weight, down_weight=down_weight)


def reference(tokens, expert_ids, gate_levels, gate_weight, up_weight, down_weight):
    shares = gate_levels.astype(jnp.float32) / 256.0
    row_limit = N_EXPERT * CAP
    count_tokens = tokens.shape[0]

    def per_expert(running, expert_index):
        matched = expert_ids == expert_index
        weight_sum = jnp.sum(jnp.where(matched, shares, jnp.float32(0.0)), axis=1)
        chosen = jnp.any(matched, axis=1)
        token_rows = jnp.nonzero(chosen, size=row_limit, fill_value=0)[0].astype(jnp.int32)
        picked = tokens[token_rows]
        gate_part = jnp.dot(picked, gate_weight[expert_index], preferred_element_type=jnp.float32)
        up_part = jnp.dot(picked, up_weight[expert_index], preferred_element_type=jnp.float32)
        hidden = (jax.nn.silu(gate_part) * up_part).astype(jnp.bfloat16)
        expert_out = jnp.dot(hidden, down_weight[expert_index], preferred_element_type=jnp.float32).astype(jnp.bfloat16)
        filled = jnp.arange(row_limit, dtype=jnp.int32) < jnp.sum(chosen.astype(jnp.int32))
        factor = jnp.where(filled, weight_sum[token_rows], jnp.float32(0.0))
        running = running.at[token_rows].add(factor[:, None] * expert_out.astype(jnp.float32))
        return running, None

    start_sum = jnp.zeros((count_tokens, tokens.shape[1]), jnp.float32)
    labels = jnp.arange(gate_weight.shape[0], dtype=jnp.int32)
    total_sum, unused = lax.scan(per_expert, start_sum, labels)
    return total_sum.astype(jnp.bfloat16)
```

```python
import functools

import jax
import jax.numpy as jnp
from jax import lax
from jax.experimental import pallas as pl
from jax.experimental.pallas import tpu as pltpu
from jax.sharding import PartitionSpec as P

MESH = pl.DeviceIdType.MESH
WIDE = 256


def slot_numbers(chosen_ids, experts, capacity):
    flat_ids = chosen_ids.reshape(-1)
    labels = jnp.arange(experts, dtype=jnp.int32)
    onehot = (flat_ids[:, None] == labels[None, :]).astype(jnp.int32)
    before = jnp.cumsum(onehot, axis=0) - onehot
    position = jnp.sum(before * onehot, axis=1)
    return (flat_ids * capacity + position).reshape(chosen_ids.shape)


def route_matrix(slots, count):
    targets = jnp.arange(count, dtype=jnp.int32)
    return jnp.any(targets[:, None, None] == slots[None, :, :], axis=2).astype(jnp.bfloat16)


def routed_on_device(tokens, expert_ids, gate_levels, gate_weight, up_weight, down_weight):
    tok_dev = tokens.shape[0]
    picks = expert_ids.shape[1]
    exp_dev = gate_weight.shape[0]
    n_expert = lax.axis_size("expert")
    experts = exp_dev * n_expert
    capacity = min(tok_dev, max(2, 2 * tok_dev * picks // experts))
    slot_count = experts * capacity
    own_slots = slot_numbers(expert_ids, experts, capacity)
    route = route_matrix(own_slots, slot_count)
    whole = lax.all_gather(tokens, "dp", axis=1, tiled=True)
    outgoing = jnp.dot(route, whole, preferred_element_type=jnp.float32).astype(jnp.bfloat16)
    outgoing = outgoing.reshape(n_expert, exp_dev, capacity, whole.shape[1])
    arrived = lax.all_to_all(outgoing, "expert", split_axis=0, concat_axis=0, tiled=True)
    gate_part = jnp.einsum(
        "sxcd,xdf->sxcf", arrived, gate_weight, preferred_element_type=jnp.float32
    )
    up_part = jnp.einsum("sxcd,xdf->sxcf", arrived, up_weight, preferred_element_type=jnp.float32)
    hidden = (jax.nn.silu(gate_part) * up_part).astype(jnp.bfloat16)
    out_features = down_weight.shape[2]
    outputs = jnp.einsum(
        "sxcf,xfk->sxck",
        lax.all_gather(hidden, "dp", axis=3, tiled=True),
        down_weight,
        preferred_element_type=jnp.float32,
    )
    result = outputs.astype(jnp.bfloat16)
    returned = lax.all_to_all(result, "expert", split_axis=0, concat_axis=0, tiled=True)
    returned = returned.reshape(slot_count, out_features)
    shares = gate_levels.astype(jnp.float32) / 256.0
    targets = jnp.arange(slot_count, dtype=jnp.int32)
    weighting = jnp.sum(
        jnp.where(
            targets[None, :, None] == own_slots[:, None, :], shares[:, None, :], jnp.float32(0.0)
        ),
        axis=2,
    )
    weighting = weighting.astype(jnp.bfloat16)
    combined = jnp.dot(weighting, returned, preferred_element_type=jnp.float32)
    return combined.astype(jnp.bfloat16)


def visit_order(chips):
    return [
        sorted(range(chips), key=lambda q: (abs(q - z), q if 2 * z < chips else -q)) for z in range(chips)
    ]


def crossings(chips, exp_dev, rows):
    piece, late = rows // 2, exp_dev - 1
    parts = [(0, "own", 0, piece, 0), (0, "own", piece, piece, 0), (0, "own", 0, piece, late), (0, "mate", 0, rows, 0)]
    for role in range(1, chips):
        for x in range(late):
            parts.append((role, "all", 0, 2 * rows, x))
        if role < 3:
            parts.append((role, "all", 0, rows, late))
            parts.append((role, "all", rows, rows, late))
        else:
            parts.append((role, "all", 0, 2 * rows, late))
    for x in range(1, exp_dev):
        parts.append((0, "mate", 0, rows, x))
    for x in range(1, late):
        parts.append((0, "own", 0, rows, x))
    parts.append((0, "own", piece, piece, late))
    return parts


def dense_kernel(
    chips, tok_hbm, ids_hbm, levels_hbm, gate_hbm, up_hbm, down_hbm, out,
    ids, levels, gate_w, up_w, down_w, x_buf, hid, acc, pair_out, pair_in, ret_out, ret_in,
    i_sem, w_sem, x_send, x_recv, c_recv, m_recv, t_send, n_send, h_send, h_recv, p_send, p_recv, r_send, r_recv,
):
    e = lax.axis_index("expert")
    d = lax.axis_index("dp")
    z, c = lax.div(e, 2), lax.rem(e, 2)
    rows, own = tok_hbm.shape
    exp_dev, depth, ff = gate_w.shape
    width = down_w.shape[2]
    tiles = width // WIDE
    piece = rows // 2
    mate = z * 2 + 1 - c

    barrier = pltpu.get_barrier_semaphore()
    pl.semaphore_signal(barrier, inc=1, device_id={"dp": 1 - d}, device_id_type=MESH)
    pl.semaphore_signal(barrier, inc=1, device_id={"expert": mate}, device_id_type=MESH)

    @pl.when(z > 0)
    def _():
        pl.semaphore_signal(barrier, inc=1, device_id={"expert": e - 2}, device_id_type=MESH)

    @pl.when(z < chips - 1)
    def _():
        pl.semaphore_signal(barrier, inc=1, device_id={"expert": e + 2}, device_id_type=MESH)

    def block(core):
        return pl.ds(pl.multiple_of(core * rows, rows), rows)

    def unit(q, core, j, h):
        at = pl.ds(pl.multiple_of(core * rows + h * piece, piece), piece)
        return x_buf.at[q, at, pl.ds(pl.multiple_of(j * own, own), own)]

    tok_loads = []
    for h in range(2):
        source = tok_hbm.at[pl.ds(h * piece, piece)]
        tok_loads.append(pltpu.make_async_copy(source, unit(z, c, d, h), i_sem.at[2 + h]))
    ids_load = pltpu.make_async_copy(ids_hbm, ids, i_sem.at[0])
    levels_load = pltpu.make_async_copy(levels_hbm, levels, i_sem.at[1])
    for load in (*tok_loads, ids_load, levels_load):
        load.start()
    loads = {}
    for x in range(exp_dev):
        for i, (source, held) in enumerate(((gate_hbm, gate_w), (up_hbm, up_w))):
            loads[i, x] = pltpu.make_async_copy(source.at[x], held.at[x], w_sem.at[x, i])
    for x in range(exp_dev):
        loads[2, x] = pltpu.make_async_copy(down_hbm.at[x], down_w.at[x], w_sem.at[x, 2])
    for load in tok_loads:
        load.wait()
    for load in loads.values():
        load.start()
    pending = set(loads)

    def loaded(*keys):
        for key in keys:
            if key in pending:
                pending.remove(key)
                loads[key].wait()

    pl.semaphore_wait(barrier, 2 + jnp.minimum(z, 1) + jnp.minimum(chips - 1 - z, 1))

    shares = pl.ds(depth, 128)

    def swap(h):
        return pltpu.make_async_remote_copy(
            src_ref=unit(z, c, d, h), dst_ref=unit(z, c, d, h),
            send_sem=n_send, recv_sem=x_recv.at[z, d, h],
            device_id={"dp": 1 - d}, device_id_type=MESH,
        )

    def push(ref, q, way, sem):
        return pltpu.make_async_remote_copy(
            src_ref=ref, dst_ref=ref, send_sem=x_send.at[q, way], recv_sem=m_recv.at[q] if way == 0 else sem,
            device_id={"expert": (mate, e + 2, e - 2)[way]}, device_id_type=MESH,
        )

    def forward(q, j, h, way):
        return push(unit(q, c, j, h), q, way, x_recv.at[q, j, h])

    def forward_share(q, way):
        return push(x_buf.at[q, block(c), shares], q, way, c_recv.at[q])

    def await_copy(ref, sem, sent=False):
        copy = pltpu.make_async_remote_copy(
            src_ref=ref, dst_ref=ref, send_sem=sem if sent else t_send, recv_sem=t_send if sent else sem,
            device_id={"expert": mate}, device_id_type=MESH,
        )
        copy.wait_send() if sent else copy.wait_recv()

    def arrived(q, j, h):
        await_copy(unit(q, c, j, h), x_recv.at[q, j, h])

    def send_all(make):
        pl.when(z < chips - 1)(lambda: make(1).start())
        pl.when(z > 0)(lambda: make(2).start())
        make(0).start()

    def send_own(j, h):
        send_all(lambda way: forward(z, j, h, way))

    def pass_on(step, make, wait):
        for way in (1, 2):
            q = z - step if way == 1 else z + step
            inside = z >= step if way == 1 else z + step < chips
            further = jnp.logical_and(inside, z < chips - 1) if way == 1 else jnp.logical_and(inside, z > 0)

            @pl.when(inside)
            def _(q=q):
                wait(q)
                make(q, 0).start()

            @pl.when(further)
            def _(q=q, way=way):
                make(q, way).start()

    def relay(step, j, h):
        pass_on(step, lambda q, way: forward(q, j, h, way), lambda q: arrived(q, j, h))

    def relay_share(step):
        pass_on(step, forward_share, lambda q: await_copy(x_buf.at[q, block(c), shares], c_recv.at[q]))

    for h in range(2):
        swap(h).start()
    for h in range(2):
        send_own(d, h)
    ids_load.wait()
    levels_load.wait()
    label = lax.broadcasted_iota(jnp.int32, (128, rows), 0)
    share = jnp.zeros((128, rows), jnp.float32)
    for k in range(ids.shape[0]):
        level = levels[k : k + 1, :].astype(jnp.float32) / 256.0
        share = share + jnp.where(ids[k : k + 1, :] == label, level, 0.0)
    x_buf[z, block(c), shares] = share.T.astype(x_buf.dtype)
    send_all(lambda way: forward_share(z, way))

    table = visit_order(chips)
    order = []
    for step in range(chips):
        q = jnp.int32(0)
        for place in range(chips):
            q = jnp.where(z == place, jnp.int32(table[place][step]), q)
        order.append(q)

    def row_range(kind, start, size):
        if kind == "all":
            return pl.ds(start, size)
        core = c if kind == "own" else 1 - c
        return pl.ds(pl.multiple_of(core * rows + start, piece), size)

    items = crossings(chips, exp_dev, rows)
    spot = {item: i for i, item in enumerate(items)}

    def piece_of(i, side, t):
        role, kind, start, size, x = items[i]
        cols = pl.ds(pl.multiple_of(side * ff + t * WIDE, WIDE), WIDE)
        return hid.at[role, x, row_range(kind, start, size), cols]

    def cross(i, t):
        return pltpu.make_async_remote_copy(
            src_ref=piece_of(i, d, t), dst_ref=piece_of(i, d, t),
            send_sem=h_send, recv_sem=h_recv.at[i],
            device_id={"dp": 1 - d}, device_id_type=MESH,
        )

    def crossed(i):
        role, kind, start, size, x = items[i]
        cols = pl.ds(pl.multiple_of((1 - d) * ff, WIDE), ff)
        await_copy(hid.at[role, x, row_range(kind, start, size), cols], h_recv.at[i])

    seen = set()
    met = set()


    def enter(role, kind, x):
        if kind != "own" and role not in seen:
            seen.add(role)
            await_copy(x_buf.at[order[role], block(1 - c)], m_recv.at[order[role]])
        loaded((0, x), (1, x))

    def release(*chosen):
        for i in chosen:
            for t in range(ff // WIDE):
                cross(i, t).start()

    def units(role, kind, start, size, x, now=(), then=()):
        enter(role, kind, x)
        at = row_range(kind, start, size)

        def finish(t, gate, up):
            put = pl.ds(pl.multiple_of(d * ff + t * WIDE, WIDE), WIDE)
            hid[role, x, at, put] = (gate / (1.0 + jnp.exp(-gate)) * up).astype(hid.dtype)
            for i in now:
                cross(i, t).start()

        held = None
        for t in range(ff // WIDE):
            cols = slice(t * WIDE, (t + 1) * WIDE)
            lhs = x_buf[order[role], at, :depth]
            gate = jnp.dot(lhs, gate_w[x, :, cols], preferred_element_type=jnp.float32)
            up = jnp.dot(lhs, up_w[x, :, cols], preferred_element_type=jnp.float32)
            if held is not None:
                finish(*held)
            held = (t, gate, up)
        finish(*held)
        release(*then)

    def hand_over(role, t):
        return pltpu.make_async_remote_copy(
            src_ref=pair_out.at[role, t], dst_ref=pair_in.at[role, t],
            send_sem=p_send, recv_sem=p_recv.at[role, t],
            device_id={"expert": mate}, device_id_type=MESH,
        )

    def give_back(role, t):
        return pltpu.make_async_remote_copy(
            src_ref=ret_out.at[role, t], dst_ref=ret_in.at[z, t],
            send_sem=r_send, recv_sem=r_recv,
            device_id={"expert": order[role] * 2 + c}, device_id_type=MESH,
        )

    def share_of(role, at, size, x):
        lanes = lax.broadcasted_iota(jnp.int32, (size, 128), 1)
        picked = jnp.where(lanes == e * exp_dev + x, x_buf[order[role], at, shares].astype(jnp.float32), 0.0)
        return jnp.sum(picked, axis=1, keepdims=True)

    def outputs(role, kind, start, size, x, side=None, first=False, last=False, turn=None):
        at = row_range(kind, start, size)
        loaded((2, x))
        weight = share_of(role, at, size, x)
        if side != "own":
            for i, (a, b, begin, count, y) in enumerate(items):
                if (a, b, y) == (role, kind, x) and begin < start + size and start < begin + count and i not in met:
                    met.add(i)
                    crossed(i)
        if side is None:
            depth_at = slice(0, 2 * ff)
        else:
            depth_at = pl.ds(pl.multiple_of((d if side == "own" else 1 - d) * ff, WIDE), ff)

        def put(t, res):
            cols = slice(t * WIDE, (t + 1) * WIDE)
            res = res * weight
            if not first:
                res = res + acc[role, at, cols]
            if not last:
                acc[role, at, cols] = res
                return
            if kind == "mate":
                pair_out[role, t] = res.astype(pair_out.dtype)
                hand_over(role, t).start()
            elif turn is None:
                acc[role, at, cols] = res
                pair_out[role, t] = acc[role, block(1 - c), cols].astype(pair_out.dtype)
                hand_over(role, t).start()
            else:
                acc[role, at, cols] = res
                slot = jnp.where(c == turn, chips, role)
                pair_out[slot, t] = res.astype(pair_out.dtype)

                @pl.when(c != turn)
                def _():
                    hand_over(role, t).start()

        held = None
        for t in range(tiles):
            cols = slice(t * WIDE, (t + 1) * WIDE)
            res = jnp.dot(hid[role, x, at, depth_at], down_w[x, depth_at, cols], preferred_element_type=jnp.float32)
            if held is not None:
                put(*held)
            held = (t, res)
        put(*held)

    def combine(role, turn=None):
        def go():
            for t in range(tiles):
                cols = slice(t * WIDE, (t + 1) * WIDE)
                hand_over(role, t).wait_recv()
                both = acc[role, block(c), cols] + pair_in[role, t].astype(jnp.float32)
                ret_out[role, t] = both.astype(ret_out.dtype)
                give_back(role, t).start()

        go() if turn is None else pl.when(c == turn)(go)

    late = exp_dev - 1
    far = chips - 1

    def remote(role, x):
        now = then = ()
        if x < late:
            now = (spot[role, "all", 0, 2 * rows, x],)
        elif role == 1:
            now = (spot[role, "all", 0, rows, x],)
        elif role > 2:
            now = (spot[role, "all", 0, 2 * rows, x],)
        units(role, "all", 0, 2 * rows, x, now=now)

    def bulk(role):
        for x in range(late):
            outputs(role, "all", 0, 2 * rows, x, first=x == 0)

    arrived(z, 1 - d, 0)
    send_own(1 - d, 0)
    units(0, "own", 0, piece, 0, now=(0,))
    arrived(z, 1 - d, 1)
    send_own(1 - d, 1)
    units(0, "own", piece, piece, 0, now=(1,))
    relay(1, d, 0)
    relay(1, d, 1)
    units(0, "own", 0, rows, late, now=(2,))
    relay_share(1)
    relay(1, 1 - d, 0)
    units(0, "mate", 0, rows, 0, now=(3,))
    relay(1, 1 - d, 1)
    for x in range(1, late):
        units(0, "own", 0, rows, x)

    for step in range(1, chips):
        more = step + 1 < chips
        for x in range(late):
            remote(step, x)
        if more:
            relay(step + 1, d, 0)
            relay(step + 1, d, 1)
        if step == 1:
            outputs(0, "own", 0, rows, 0, first=True)
        if more:
            relay(step + 1, 1 - d, 0)
        remote(step, late)
        if more:
            relay_share(step + 1)
        if step == 1:
            outputs(0, "mate", 0, rows, 0, first=True)
        if more:
            relay(step + 1, 1 - d, 1)
        if step == 2:
            bulk(1)
            outputs(1, "all", 0, rows, late, last=True, turn=0)
        if step == 3:
            combine(1, 0)
        if step == 4:
            bulk(2)
        if step > 4:
            bulk(step - 2)
            outputs(step - 2, "all", 0, 2 * rows, late, last=True)
            combine(step - 2)
    release(spot[2, "all", 0, rows, late], spot[2, "all", rows, rows, late], spot[1, "all", rows, rows, late])
    for x in range(1, exp_dev):
        units(0, "mate", 0, rows, x, now=(spot[0, "mate", 0, rows, x],))
    release(*(spot[0, "own", 0, rows, x] for x in range(1, late)), spot[0, "own", piece, piece, late])
    if chips == 3:
        combine(1, 0)
    if chips < 5:
        bulk(2)
    if chips > 4:
        bulk(far - 1)
        outputs(far - 1, "all", 0, 2 * rows, late, last=True)
        combine(far - 1)
    if far > 2:
        bulk(far)
        outputs(far, "all", 0, 2 * rows, late, last=True)
    outputs(2, "all", 0, 2 * rows, late, side="own")
    outputs(1, "all", rows, rows, late, side="own")
    if far > 2:
        combine(far)
    for x in range(1, exp_dev):
        outputs(0, "mate", 0, rows, x, side="own")
        outputs(0, "own", 0, rows, x, side="own")
    for turn in range(2):
        outputs(2, "all", turn * rows, rows, late, side="other", last=True, turn=turn)
    for turn in range(2):
        combine(2, turn)
    outputs(1, "all", rows, rows, late, side="other", last=True, turn=1)
    for x in range(1, late):
        outputs(0, "mate", 0, rows, x, side="other")
    combine(1, 1)
    outputs(0, "mate", 0, rows, late, side="other", last=True)
    for x in range(1, exp_dev):
        outputs(0, "own", 0, rows, x, side="other")

    for t in range(tiles):
        hand_over(0, t).wait_recv()
    await_copy(ret_in.at[pl.ds(0, chips - 1)], r_recv)
    for t in range(tiles):
        cols = slice(t * WIDE, (t + 1) * WIDE)
        full = acc[0, block(c), cols] + pair_in[0, t].astype(jnp.float32)
        for i in range(1, chips):
            full = full + ret_in[lax.rem(z + i, chips), t].astype(jnp.float32)
        out[:, cols] = full.astype(out.dtype)

    await_copy(x_buf.at[z, block(c), pl.ds(pl.multiple_of(d * own, own), own)], n_send, sent=True)
    for q in range(chips):
        await_copy(x_buf.at[q, block(c)], x_send.at[q, 0], sent=True)
        for way, sends in ((1, jnp.logical_and(q <= z, z < chips - 1)), (2, jnp.logical_and(q >= z, z > 0))):
            @pl.when(sends)
            def _(q=q, way=way):
                await_copy(x_buf.at[q, block(c)], x_send.at[q, way], sent=True)
    await_copy(hid.at[:, :, :, pl.ds(pl.multiple_of(d * ff, WIDE), ff)], h_send, sent=True)
    await_copy(pair_out.at[pl.ds(0, chips)], p_send, sent=True)
    await_copy(ret_out.at[pl.ds(1, chips - 1)], r_send, sent=True)


def dense_on_device(tokens, expert_ids, gate_levels, gate_weight, up_weight, down_weight):
    chips = lax.axis_size("expert") // 2
    rows, own = tokens.shape
    exp_dev, depth, ff = gate_weight.shape
    width = down_weight.shape[2]
    kind = tokens.dtype
    tiles = width // WIDE
    picks = expert_ids.shape[1]
    count = len(crossings(chips, exp_dev, rows))
    anywhere = pl.BlockSpec(memory_space=pl.ANY)
    dma = pltpu.SemaphoreType.DMA
    operands = [
        pltpu.with_memory_space_constraint(a, memory_space=pltpu.HBM)
        for a in (tokens, expert_ids.T, gate_levels.T, gate_weight, up_weight, down_weight)
    ]
    flops = 2 * chips * 2 * rows * exp_dev * (2 * depth * ff + 2 * ff * width)
    return pl.pallas_call(
        functools.partial(dense_kernel, chips),
        out_shape=jax.ShapeDtypeStruct((rows, width), kind),
        in_specs=[anywhere] * 6,
        out_specs=pl.BlockSpec(memory_space=pltpu.VMEM),
        scratch_shapes=[
            pltpu.VMEM((picks, rows), jnp.int32),
            pltpu.VMEM((picks, rows), jnp.int32),
            pltpu.VMEM(gate_weight.shape, kind),
            pltpu.VMEM(up_weight.shape, kind),
            pltpu.VMEM(down_weight.shape, kind),
            pltpu.VMEM((chips, 2 * rows, depth + 128), kind),
            pltpu.VMEM((chips, exp_dev, 2 * rows, 2 * ff), kind),
            pltpu.VMEM((chips, 2 * rows, width), jnp.float32),
            pltpu.VMEM((chips + 1, tiles, rows, WIDE), kind),
            pltpu.VMEM((chips, tiles, rows, WIDE), kind),
            pltpu.VMEM((chips, tiles, rows, WIDE), kind),
            pltpu.VMEM((chips, tiles, rows, WIDE), kind),
            dma((4,)),
            dma((exp_dev, 3)),
            dma((chips, 3)),
            dma((chips, 2, 2)),
            dma((chips,)),
            dma((chips,)),
            dma,
            dma,
            dma,
            dma((count,)),
            dma,
            dma((chips, tiles)),
            dma,
            dma,
        ],
        compiler_params=pltpu.CompilerParams(
            collective_id=0, has_side_effects=True, vmem_limit_bytes=50331648
        ),
        cost_estimate=pl.CostEstimate(
            flops=flops, bytes_accessed=2 * 3 * gate_weight.size, transcendentals=0
        ),
    )(*operands)


def on_device(tokens, expert_ids, gate_levels, gate_weight, up_weight, down_weight):
    rows, own = tokens.shape
    exp_dev, depth, ff = gate_weight.shape
    n_expert = lax.axis_size("expert")
    width = down_weight.shape[2]
    experts = exp_dev * n_expert
    dense = (
        2 * rows * expert_ids.shape[1] >= rows * experts
        and lax.axis_size("dp") == 2
        and n_expert % 2 == 0
        and n_expert >= 6
        and experts <= 128
        and rows % 32 == 0
        and exp_dev >= 2
        and own % 128 == 0
        and ff % WIDE == 0
        and width % WIDE == 0
    )
    call = dense_on_device if dense else routed_on_device
    return call(tokens, expert_ids, gate_levels, gate_weight, up_weight, down_weight)


def solution(mesh):
    in_specs = (
        P(("groups", "expert"), "dp"),
        P(("groups", "expert"), None),
        P(("groups", "expert"), None),
        P("expert", None, "dp"),
        P("expert", None, "dp"),
        P("expert", None, "dp"),
    )
    out_specs = P(("groups", "expert"), "dp")
    return jax.shard_map(
        on_device, mesh=mesh, in_specs=in_specs, out_specs=out_specs, check_vma=False
    )
```

```python
import functools

import jax
import jax.numpy as jnp
from jax import lax
from jax.experimental import pallas as pl
from jax.experimental.pallas import tpu as pltpu
from jax.sharding import PartitionSpec as P

MESH = pl.DeviceIdType.MESH
WIDE = 256


def slot_numbers(chosen_ids, experts, capacity):
    flat_ids = chosen_ids.reshape(-1)
    labels = jnp.arange(experts, dtype=jnp.int32)
    onehot = (flat_ids[:, None] == labels[None, :]).astype(jnp.int32)
    before = jnp.cumsum(onehot, axis=0) - onehot
    position = jnp.sum(before * onehot, axis=1)
    return (flat_ids * capacity + position).reshape(chosen_ids.shape)


def route_matrix(slots, count):
    targets = jnp.arange(count, dtype=jnp.int32)
    return jnp.any(targets[:, None, None] == slots[None, :, :], axis=2).astype(jnp.bfloat16)


def routed_on_device(tokens, expert_ids, gate_levels, gate_weight, up_weight, down_weight):
    tok_dev = tokens.shape[0]
    picks = expert_ids.shape[1]
    exp_dev = gate_weight.shape[0]
    n_expert = lax.axis_size("expert")
    experts = exp_dev * n_expert
    capacity = min(tok_dev, max(2, 2 * tok_dev * picks // experts))
    slot_count = experts * capacity
    own_slots = slot_numbers(expert_ids, experts, capacity)
    route = route_matrix(own_slots, slot_count)
    whole = lax.all_gather(tokens, "dp", axis=1, tiled=True)
    outgoing = jnp.dot(route, whole, preferred_element_type=jnp.float32).astype(jnp.bfloat16)
    outgoing = outgoing.reshape(n_expert, exp_dev, capacity, whole.shape[1])
    arrived = lax.all_to_all(outgoing, "expert", split_axis=0, concat_axis=0, tiled=True)
    gate_part = jnp.einsum(
        "sxcd,xdf->sxcf", arrived, gate_weight, preferred_element_type=jnp.float32
    )
    up_part = jnp.einsum("sxcd,xdf->sxcf", arrived, up_weight, preferred_element_type=jnp.float32)
    hidden = (jax.nn.silu(gate_part) * up_part).astype(jnp.bfloat16)
    out_features = down_weight.shape[2]
    outputs = jnp.einsum(
        "sxcf,xfk->sxck",
        lax.all_gather(hidden, "dp", axis=3, tiled=True),
        down_weight,
        preferred_element_type=jnp.float32,
    )
    result = outputs.astype(jnp.bfloat16)
    returned = lax.all_to_all(result, "expert", split_axis=0, concat_axis=0, tiled=True)
    returned = returned.reshape(slot_count, out_features)
    shares = gate_levels.astype(jnp.float32) / 256.0
    targets = jnp.arange(slot_count, dtype=jnp.int32)
    weighting = jnp.sum(
        jnp.where(
            targets[None, :, None] == own_slots[:, None, :], shares[:, None, :], jnp.float32(0.0)
        ),
        axis=2,
    )
    weighting = weighting.astype(jnp.bfloat16)
    combined = jnp.dot(weighting, returned, preferred_element_type=jnp.float32)
    return combined.astype(jnp.bfloat16)


def visit_order(chips):
    table = []
    for z in range(chips):
        up = 2 * z < chips
        inward = sorted((q for q in range(chips) if q != z and (q > z) == up), key=lambda q: abs(q - z))
        outward = sorted((q for q in range(chips) if q != z and (q > z) != up), key=lambda q: -abs(q - z))
        table.append([z, *inward, *outward])
    return table


def crossings(chips, exp_dev, rows):
    piece, late = rows // 2, exp_dev - 1
    parts = [(0, "own", 0, piece, 0), (0, "own", piece, piece, 0), (0, "own", 0, piece, late), (0, "mate", 0, rows, 0)]
    for x in range(late):
        parts.append((1, "all", 0, 2 * rows, x))
    for turn in range(2):
        parts.append((1, "all", turn * rows, rows, late))
    for role in range(2, chips):
        for turn in range(2):
            for x in range(exp_dev):
                parts.append((role, "all", turn * rows, rows, x))
    for x in range(1, exp_dev):
        parts.append((0, "mate", 0, rows, x))
    for x in range(1, late):
        parts.append((0, "own", 0, rows, x))
    parts.append((0, "own", piece, piece, late))
    return parts


def dense_kernel(
    chips, tok_hbm, ids_hbm, levels_hbm, gate_hbm, up_hbm, down_hbm, out,
    ids, levels, gate_w, up_w, down_w, x_buf, hid, acc, pair_out, pair_in, ret_out, ret_in,
    i_sem, w_sem, x_send, x_recv, c_recv, m_recv, t_send, n_send, h_send, h_recv, p_send, p_recv, r_send, r_recv,
):
    e = lax.axis_index("expert")
    d = lax.axis_index("dp")
    z, c = lax.div(e, 2), lax.rem(e, 2)
    rows, own = tok_hbm.shape
    exp_dev, depth, ff = gate_w.shape
    width = down_w.shape[2]
    tiles = width // WIDE
    piece = rows // 2
    mate = z * 2 + 1 - c

    barrier = pltpu.get_barrier_semaphore()
    pl.semaphore_signal(barrier, inc=1, device_id={"dp": 1 - d}, device_id_type=MESH)
    pl.semaphore_signal(barrier, inc=1, device_id={"expert": mate}, device_id_type=MESH)

    @pl.when(z > 0)
    def _():
        pl.semaphore_signal(barrier, inc=1, device_id={"expert": e - 2}, device_id_type=MESH)

    @pl.when(z < chips - 1)
    def _():
        pl.semaphore_signal(barrier, inc=1, device_id={"expert": e + 2}, device_id_type=MESH)

    def block(core):
        return pl.ds(pl.multiple_of(core * rows, rows), rows)

    def unit(q, core, j, h):
        at = pl.ds(pl.multiple_of(core * rows + h * piece, piece), piece)
        return x_buf.at[q, at, pl.ds(pl.multiple_of(j * own, own), own)]

    tok_loads = []
    for h in range(2):
        source = tok_hbm.at[pl.ds(h * piece, piece)]
        tok_loads.append(pltpu.make_async_copy(source, unit(z, c, d, h), i_sem.at[2 + h]))
    ids_load = pltpu.make_async_copy(ids_hbm, ids, i_sem.at[0])
    levels_load = pltpu.make_async_copy(levels_hbm, levels, i_sem.at[1])
    for load in (*tok_loads, ids_load, levels_load):
        load.start()
    loads = {}
    for x in range(exp_dev):
        for i, (source, held) in enumerate(((gate_hbm, gate_w), (up_hbm, up_w))):
            loads[i, x] = pltpu.make_async_copy(source.at[x], held.at[x], w_sem.at[x, i])
    for x in range(exp_dev):
        loads[2, x] = pltpu.make_async_copy(down_hbm.at[x], down_w.at[x], w_sem.at[x, 2])
    for load in tok_loads:
        load.wait()
    for load in loads.values():
        load.start()
    pending = set(loads)

    def loaded(*keys):
        for key in keys:
            if key in pending:
                pending.remove(key)
                loads[key].wait()

    pl.semaphore_wait(barrier, 2 + jnp.minimum(z, 1) + jnp.minimum(chips - 1 - z, 1))

    shares = pl.ds(depth, 128)

    def swap(h):
        return pltpu.make_async_remote_copy(
            src_ref=unit(z, c, d, h), dst_ref=unit(z, c, d, h),
            send_sem=n_send, recv_sem=x_recv.at[z, d, h],
            device_id={"dp": 1 - d}, device_id_type=MESH,
        )

    def push(ref, q, way, sem):
        return pltpu.make_async_remote_copy(
            src_ref=ref, dst_ref=ref, send_sem=x_send.at[q, way], recv_sem=m_recv.at[q] if way == 0 else sem,
            device_id={"expert": (mate, e + 2, e - 2)[way]}, device_id_type=MESH,
        )

    def forward(q, j, h, way):
        return push(unit(q, c, j, h), q, way, x_recv.at[q, j, h])

    def forward_share(q, way):
        return push(x_buf.at[q, block(c), shares], q, way, c_recv.at[q])

    def await_copy(ref, sem, sent=False):
        copy = pltpu.make_async_remote_copy(
            src_ref=ref, dst_ref=ref, send_sem=sem if sent else t_send, recv_sem=t_send if sent else sem,
            device_id={"expert": mate}, device_id_type=MESH,
        )
        copy.wait_send() if sent else copy.wait_recv()

    def arrived(q, j, h):
        await_copy(unit(q, c, j, h), x_recv.at[q, j, h])

    def send_all(make):
        pl.when(z < chips - 1)(lambda: make(1).start())
        pl.when(z > 0)(lambda: make(2).start())
        make(0).start()

    def send_own(j, h):
        send_all(lambda way: forward(z, j, h, way))

    def pass_on(step, make, wait):
        for way in (1, 2):
            q = z - step if way == 1 else z + step
            inside = z >= step if way == 1 else z + step < chips
            further = jnp.logical_and(inside, z < chips - 1) if way == 1 else jnp.logical_and(inside, z > 0)

            @pl.when(inside)
            def _(q=q):
                wait(q)
                make(q, 0).start()

            @pl.when(further)
            def _(q=q, way=way):
                make(q, way).start()

    def relay(step, j, h):
        pass_on(step, lambda q, way: forward(q, j, h, way), lambda q: arrived(q, j, h))

    def relay_share(step):
        pass_on(step, forward_share, lambda q: await_copy(x_buf.at[q, block(c), shares], c_recv.at[q]))

    for h in range(2):
        swap(h).start()
    for h in range(2):
        send_own(d, h)
    ids_load.wait()
    levels_load.wait()
    label = lax.broadcasted_iota(jnp.int32, (128, rows), 0)
    share = jnp.zeros((128, rows), jnp.float32)
    for k in range(ids.shape[0]):
        level = levels[k : k + 1, :].astype(jnp.float32) / 256.0
        share = share + jnp.where(ids[k : k + 1, :] == label, level, 0.0)
    x_buf[z, block(c), shares] = share.T.astype(x_buf.dtype)
    send_all(lambda way: forward_share(z, way))

    table = visit_order(chips)
    order = []
    for step in range(chips):
        q = jnp.int32(0)
        for place in range(chips):
            q = jnp.where(z == place, jnp.int32(table[place][step]), q)
        order.append(q)

    def row_range(kind, start, size):
        if kind == "all":
            return pl.ds(start, size)
        core = c if kind == "own" else 1 - c
        return pl.ds(pl.multiple_of(core * rows + start, piece), size)

    items = crossings(chips, exp_dev, rows)
    spot = {item: i for i, item in enumerate(items)}

    def piece_of(i, side, t):
        role, kind, start, size, x = items[i]
        cols = pl.ds(pl.multiple_of(side * ff + t * WIDE, WIDE), WIDE)
        return hid.at[role, x, row_range(kind, start, size), cols]

    def cross(i, t):
        return pltpu.make_async_remote_copy(
            src_ref=piece_of(i, d, t), dst_ref=piece_of(i, d, t),
            send_sem=h_send, recv_sem=h_recv.at[i],
            device_id={"dp": 1 - d}, device_id_type=MESH,
        )

    def crossed(i):
        role, kind, start, size, x = items[i]
        cols = pl.ds(pl.multiple_of((1 - d) * ff, WIDE), ff)
        await_copy(hid.at[role, x, row_range(kind, start, size), cols], h_recv.at[i])

    seen = set()
    met = set()


    def enter(role, kind, x):
        if kind != "own" and role not in seen:
            seen.add(role)
            await_copy(x_buf.at[order[role], block(1 - c)], m_recv.at[order[role]])
        loaded((0, x), (1, x))

    def release(*chosen):
        for i in chosen:
            for t in range(ff // WIDE):
                cross(i, t).start()

    def units(role, kind, start, size, x, now=(), then=()):
        enter(role, kind, x)
        at = row_range(kind, start, size)

        def finish(t, gate, up):
            put = pl.ds(pl.multiple_of(d * ff + t * WIDE, WIDE), WIDE)
            hid[role, x, at, put] = (gate / (1.0 + jnp.exp(-gate)) * up).astype(hid.dtype)
            for i in now:
                cross(i, t).start()

        held = None
        for t in range(ff // WIDE):
            cols = slice(t * WIDE, (t + 1) * WIDE)
            lhs = x_buf[order[role], at, :depth]
            gate = jnp.dot(lhs, gate_w[x, :, cols], preferred_element_type=jnp.float32)
            up = jnp.dot(lhs, up_w[x, :, cols], preferred_element_type=jnp.float32)
            if held is not None:
                finish(*held)
            held = (t, gate, up)
        finish(*held)
        release(*then)

    def hand_over(role, t):
        return pltpu.make_async_remote_copy(
            src_ref=pair_out.at[role, t], dst_ref=pair_in.at[role, t],
            send_sem=p_send, recv_sem=p_recv.at[role, t],
            device_id={"expert": mate}, device_id_type=MESH,
        )

    def give_back(role, t):
        return pltpu.make_async_remote_copy(
            src_ref=ret_out.at[role, t], dst_ref=ret_in.at[z, t],
            send_sem=r_send, recv_sem=r_recv,
            device_id={"expert": order[role] * 2 + c}, device_id_type=MESH,
        )

    def share_of(role, at, size, x):
        lanes = lax.broadcasted_iota(jnp.int32, (size, 128), 1)
        picked = jnp.where(lanes == e * exp_dev + x, x_buf[order[role], at, shares].astype(jnp.float32), 0.0)
        return jnp.sum(picked, axis=1, keepdims=True)

    def outputs(role, kind, start, size, x, side=None, first=False, last=False, turn=None):
        at = row_range(kind, start, size)
        loaded((2, x))
        weight = share_of(role, at, size, x)
        if side != "own":
            for i, (a, b, begin, count, y) in enumerate(items):
                if (a, b, y) == (role, kind, x) and begin < start + size and start < begin + count and i not in met:
                    met.add(i)
                    crossed(i)
        if side is None:
            depth_at = slice(0, 2 * ff)
        else:
            depth_at = pl.ds(pl.multiple_of((d if side == "own" else 1 - d) * ff, WIDE), ff)

        def put(t, res):
            cols = slice(t * WIDE, (t + 1) * WIDE)
            res = res * weight
            if not first:
                res = res + acc[role, at, cols]
            if not last:
                acc[role, at, cols] = res
                return
            if kind == "mate":
                pair_out[role, t] = res.astype(pair_out.dtype)
                hand_over(role, t).start()
            elif turn is None:
                acc[role, at, cols] = res
                pair_out[role, t] = acc[role, block(1 - c), cols].astype(pair_out.dtype)
                hand_over(role, t).start()
            else:
                acc[role, at, cols] = res
                slot = jnp.where(c == turn, chips, role)
                pair_out[slot, t] = res.astype(pair_out.dtype)

                @pl.when(c != turn)
                def _():
                    hand_over(role, t).start()

        held = None
        for t in range(tiles):
            cols = slice(t * WIDE, (t + 1) * WIDE)
            res = jnp.dot(hid[role, x, at, depth_at], down_w[x, depth_at, cols], preferred_element_type=jnp.float32)
            if held is not None:
                put(*held)
            held = (t, res)
        put(*held)

    def combine(role, turn=None):
        def go():
            for t in range(tiles):
                cols = slice(t * WIDE, (t + 1) * WIDE)
                hand_over(role, t).wait_recv()
                both = acc[role, block(c), cols] + pair_in[role, t].astype(jnp.float32)
                ret_out[role, t] = both.astype(ret_out.dtype)
                give_back(role, t).start()

        go() if turn is None else pl.when(c == turn)(go)

    late = exp_dev - 1
    far = chips - 1

    def remote(role, x):
        if role == 1 and x < late:
            units(role, "all", 0, 2 * rows, x, now=(spot[role, "all", 0, 2 * rows, x],))
            return
        then = (spot[role, "all", rows, rows, y] for y in range(exp_dev)) if role > 1 and x == late else ()
        units(role, "all", 0, 2 * rows, x, now=(spot[role, "all", 0, rows, x],), then=then)

    def half(role, turn, side=None):
        for x in range(exp_dev):
            first = x == 0 and side is None
            outputs(role, "all", turn * rows, rows, x, side=side, first=first, last=x == late, turn=turn)

    arrived(z, 1 - d, 0)
    send_own(1 - d, 0)
    units(0, "own", 0, piece, 0, now=(0,))
    arrived(z, 1 - d, 1)
    send_own(1 - d, 1)
    units(0, "own", piece, piece, 0, now=(1,))
    units(0, "own", 0, rows, late, now=(2,))
    relay(1, d, 0)
    relay(1, d, 1)
    relay_share(1)
    relay(1, 1 - d, 0)
    units(0, "mate", 0, rows, 0, now=(3,))
    relay(1, 1 - d, 1)
    for x in range(1, late):
        units(0, "own", 0, rows, x)

    for step in range(1, chips):
        more = step + 1 < chips
        for x in range(late):
            remote(step, x)
        if step > 1:
            remote(step, late)
        if more:
            relay(step + 1, d, 0)
            relay(step + 1, d, 1)
        if step == 1:
            outputs(0, "own", 0, rows, 0, first=True)
        if more:
            relay(step + 1, 1 - d, 0)
        if step == 1:
            remote(step, late)
        if more:
            relay_share(step + 1)
        if step == 1:
            outputs(0, "mate", 0, rows, 0, first=True)
        if more:
            relay(step + 1, 1 - d, 1)
        if step > 3:
            for turn in range(2):
                half(step - 2, turn)
            for turn in range(2):
                combine(step - 2, turn)
    release(spot[1, "all", rows, rows, late])
    for x in range(1, exp_dev):
        units(0, "mate", 0, rows, x, now=(spot[0, "mate", 0, rows, x],))
    release(*(spot[0, "own", 0, rows, x] for x in range(1, late)), spot[0, "own", piece, piece, late])
    for x in range(late):
        outputs(1, "all", 0, 2 * rows, x, first=x == 0)
    outputs(1, "all", 0, rows, late, last=True, turn=0)
    if far > 2:
        half(far - 1, 0)
    combine(1, 0)
    if far > 2:
        combine(far - 1, 0)
        half(far - 1, 1)
    for x in range(exp_dev):
        outputs(far, "all", 0, 2 * rows, x, side="own", first=x == 0)
    if far > 2:
        combine(far - 1, 1)
    outputs(1, "all", rows, rows, late, side="own")
    for x in range(1, exp_dev):
        outputs(0, "mate", 0, rows, x, side="own")
        outputs(0, "own", 0, rows, x, side="own")
    half(far, 0, side="other")
    for x in range(late):
        outputs(far, "all", rows, rows, x, side="other")
    combine(far, 0)
    outputs(far, "all", rows, rows, late, side="other", last=True, turn=1)
    combine(far, 1)
    outputs(1, "all", rows, rows, late, side="other", last=True, turn=1)
    for x in range(1, late):
        outputs(0, "mate", 0, rows, x, side="other")
    combine(1, 1)
    outputs(0, "mate", 0, rows, late, side="other", last=True)
    for x in range(1, exp_dev):
        outputs(0, "own", 0, rows, x, side="other")

    for t in range(tiles):
        hand_over(0, t).wait_recv()
    await_copy(ret_in.at[pl.ds(0, chips - 1)], r_recv)
    for t in range(tiles):
        cols = slice(t * WIDE, (t + 1) * WIDE)
        full = acc[0, block(c), cols] + pair_in[0, t].astype(jnp.float32)
        for i in range(1, chips):
            full = full + ret_in[lax.rem(z + i, chips), t].astype(jnp.float32)
        out[:, cols] = full.astype(out.dtype)

    await_copy(x_buf.at[z, block(c), pl.ds(pl.multiple_of(d * own, own), own)], n_send, sent=True)
    for q in range(chips):
        await_copy(x_buf.at[q, block(c)], x_send.at[q, 0], sent=True)
        for way, sends in ((1, jnp.logical_and(q <= z, z < chips - 1)), (2, jnp.logical_and(q >= z, z > 0))):
            @pl.when(sends)
            def _(q=q, way=way):
                await_copy(x_buf.at[q, block(c)], x_send.at[q, way], sent=True)
    await_copy(hid.at[:, :, :, pl.ds(pl.multiple_of(d * ff, WIDE), ff)], h_send, sent=True)
    await_copy(pair_out.at[pl.ds(0, chips)], p_send, sent=True)
    await_copy(ret_out.at[pl.ds(1, chips - 1)], r_send, sent=True)


def dense_on_device(tokens, expert_ids, gate_levels, gate_weight, up_weight, down_weight):
    chips = lax.axis_size("expert") // 2
    rows, own = tokens.shape
    exp_dev, depth, ff = gate_weight.shape
    width = down_weight.shape[2]
    kind = tokens.dtype
    tiles = width // WIDE
    picks = expert_ids.shape[1]
    count = len(crossings(chips, exp_dev, rows))
    anywhere = pl.BlockSpec(memory_space=pl.ANY)
    dma = pltpu.SemaphoreType.DMA
    operands = [
        pltpu.with_memory_space_constraint(a, memory_space=pltpu.HBM)
        for a in (tokens, expert_ids.T, gate_levels.T, gate_weight, up_weight, down_weight)
    ]
    flops = 2 * chips * 2 * rows * exp_dev * (2 * depth * ff + 2 * ff * width)
    return pl.pallas_call(
        functools.partial(dense_kernel, chips),
        out_shape=jax.ShapeDtypeStruct((rows, width), kind),
        in_specs=[anywhere] * 6,
        out_specs=pl.BlockSpec(memory_space=pltpu.VMEM),
        scratch_shapes=[
            pltpu.VMEM((picks, rows), jnp.int32),
            pltpu.VMEM((picks, rows), jnp.int32),
            pltpu.VMEM(gate_weight.shape, kind),
            pltpu.VMEM(up_weight.shape, kind),
            pltpu.VMEM(down_weight.shape, kind),
            pltpu.VMEM((chips, 2 * rows, depth + 128), kind),
            pltpu.VMEM((chips, exp_dev, 2 * rows, 2 * ff), kind),
            pltpu.VMEM((chips, 2 * rows, width), jnp.float32),
            pltpu.VMEM((chips + 1, tiles, rows, WIDE), kind),
            pltpu.VMEM((chips, tiles, rows, WIDE), kind),
            pltpu.VMEM((chips, tiles, rows, WIDE), kind),
            pltpu.VMEM((chips, tiles, rows, WIDE), kind),
            dma((4,)),
            dma((exp_dev, 3)),
            dma((chips, 3)),
            dma((chips, 2, 2)),
            dma((chips,)),
            dma((chips,)),
            dma,
            dma,
            dma,
            dma((count,)),
            dma,
            dma((chips, tiles)),
            dma,
            dma,
        ],
        compiler_params=pltpu.CompilerParams(
            collective_id=0, has_side_effects=True, vmem_limit_bytes=50331648
        ),
        cost_estimate=pl.CostEstimate(
            flops=flops, bytes_accessed=2 * 3 * gate_weight.size, transcendentals=0
        ),
    )(*operands)


def on_device(tokens, expert_ids, gate_levels, gate_weight, up_weight, down_weight):
    rows, own = tokens.shape
    exp_dev, depth, ff = gate_weight.shape
    n_expert = lax.axis_size("expert")
    width = down_weight.shape[2]
    experts = exp_dev * n_expert
    dense = (
        2 * rows * expert_ids.shape[1] >= rows * experts
        and lax.axis_size("dp") == 2
        and n_expert % 2 == 0
        and n_expert >= 6
        and experts <= 128
        and rows % 32 == 0
        and exp_dev >= 2
        and own % 128 == 0
        and ff % WIDE == 0
        and width % WIDE == 0
    )
    call = dense_on_device if dense else routed_on_device
    return call(tokens, expert_ids, gate_levels, gate_weight, up_weight, down_weight)


def solution(mesh):
    in_specs = (
        P(("groups", "expert"), "dp"),
        P(("groups", "expert"), None),
        P(("groups", "expert"), None),
        P("expert", None, "dp"),
        P("expert", None, "dp"),
        P("expert", None, "dp"),
    )
    out_specs = P(("groups", "expert"), "dp")
    return jax.shard_map(
        on_device, mesh=mesh, in_specs=in_specs, out_specs=out_specs, check_vma=False
    )
```

```python
import functools

import jax
import jax.numpy as jnp
from jax import lax
from jax.experimental import pallas as pl
from jax.experimental.pallas import tpu as pltpu
from jax.sharding import PartitionSpec as P

MESH = pl.DeviceIdType.MESH
WIDE = 256


def slot_numbers(chosen_ids, experts, capacity):
    flat_ids = chosen_ids.reshape(-1)
    labels = jnp.arange(experts, dtype=jnp.int32)
    onehot = (flat_ids[:, None] == labels[None, :]).astype(jnp.int32)
    before = jnp.cumsum(onehot, axis=0) - onehot
    position = jnp.sum(before * onehot, axis=1)
    return (flat_ids * capacity + position).reshape(chosen_ids.shape)


def route_matrix(slots, count):
    targets = jnp.arange(count, dtype=jnp.int32)
    return jnp.any(targets[:, None, None] == slots[None, :, :], axis=2).astype(jnp.bfloat16)


def routed_on_device(tokens, expert_ids, gate_levels, gate_weight, up_weight, down_weight):
    tok_dev = tokens.shape[0]
    picks = expert_ids.shape[1]
    exp_dev = gate_weight.shape[0]
    n_expert = lax.axis_size("expert")
    experts = exp_dev * n_expert
    capacity = min(tok_dev, max(2, 2 * tok_dev * picks // experts))
    slot_count = experts * capacity
    own_slots = slot_numbers(expert_ids, experts, capacity)
    route = route_matrix(own_slots, slot_count)
    whole = lax.all_gather(tokens, "dp", axis=1, tiled=True)
    outgoing = jnp.dot(route, whole, preferred_element_type=jnp.float32).astype(jnp.bfloat16)
    outgoing = outgoing.reshape(n_expert, exp_dev, capacity, whole.shape[1])
    arrived = lax.all_to_all(outgoing, "expert", split_axis=0, concat_axis=0, tiled=True)
    gate_part = jnp.einsum(
        "sxcd,xdf->sxcf", arrived, gate_weight, preferred_element_type=jnp.float32
    )
    up_part = jnp.einsum("sxcd,xdf->sxcf", arrived, up_weight, preferred_element_type=jnp.float32)
    hidden = (jax.nn.silu(gate_part) * up_part).astype(jnp.bfloat16)
    out_features = down_weight.shape[2]
    outputs = jnp.einsum(
        "sxcf,xfk->sxck",
        lax.all_gather(hidden, "dp", axis=3, tiled=True),
        down_weight,
        preferred_element_type=jnp.float32,
    )
    result = outputs.astype(jnp.bfloat16)
    returned = lax.all_to_all(result, "expert", split_axis=0, concat_axis=0, tiled=True)
    returned = returned.reshape(slot_count, out_features)
    shares = gate_levels.astype(jnp.float32) / 256.0
    targets = jnp.arange(slot_count, dtype=jnp.int32)
    weighting = jnp.sum(
        jnp.where(
            targets[None, :, None] == own_slots[:, None, :], shares[:, None, :], jnp.float32(0.0)
        ),
        axis=2,
    )
    weighting = weighting.astype(jnp.bfloat16)
    combined = jnp.dot(weighting, returned, preferred_element_type=jnp.float32)
    return combined.astype(jnp.bfloat16)


def visit_order(chips):
    table = []
    for z in range(chips):
        up = 2 * z < chips
        inward = sorted((q for q in range(chips) if q != z and (q > z) == up), key=lambda q: abs(q - z))
        outward = sorted((q for q in range(chips) if q != z and (q > z) != up), key=lambda q: -abs(q - z))
        table.append([z, *inward, *outward])
    return table


def crossings(chips, exp_dev, rows):
    piece, late = rows // 2, exp_dev - 1
    parts = [(0, "own", 0, piece, 0), (0, "own", piece, piece, 0), (0, "own", 0, piece, late), (0, "mate", 0, rows, 0)]
    for x in range(late):
        parts.append((1, "all", 0, 2 * rows, x))
    for turn in range(2):
        parts.append((1, "all", turn * rows, rows, late))
    for role in range(2, chips):
        for turn in range(2):
            for x in range(exp_dev):
                parts.append((role, "all", turn * rows, rows, x))
    for x in range(1, exp_dev):
        parts.append((0, "mate", 0, rows, x))
    for x in range(1, late):
        parts.append((0, "own", 0, rows, x))
    parts.append((0, "own", piece, piece, late))
    return parts


def dense_kernel(
    chips, tok_hbm, ids_hbm, levels_hbm, gate_hbm, up_hbm, down_hbm, out,
    ids, levels, gate_w, up_w, down_w, x_buf, hid, acc, pair_out, pair_in, ret_out, ret_in,
    i_sem, w_sem, x_send, x_recv, c_recv, m_recv, t_send, n_send, h_send, h_recv, p_send, p_recv, r_send, r_recv,
):
    e = lax.axis_index("expert")
    d = lax.axis_index("dp")
    z, c = lax.div(e, 2), lax.rem(e, 2)
    rows, own = tok_hbm.shape
    exp_dev, depth, ff = gate_w.shape
    width = down_w.shape[2]
    tiles = width // WIDE
    piece = rows // 2
    mate = z * 2 + 1 - c

    barrier = pltpu.get_barrier_semaphore()
    pl.semaphore_signal(barrier, inc=1, device_id={"dp": 1 - d}, device_id_type=MESH)
    pl.semaphore_signal(barrier, inc=1, device_id={"expert": mate}, device_id_type=MESH)

    @pl.when(z > 0)
    def _():
        pl.semaphore_signal(barrier, inc=1, device_id={"expert": e - 2}, device_id_type=MESH)

    @pl.when(z < chips - 1)
    def _():
        pl.semaphore_signal(barrier, inc=1, device_id={"expert": e + 2}, device_id_type=MESH)

    def block(core):
        return pl.ds(pl.multiple_of(core * rows, rows), rows)

    def unit(q, core, j, h):
        at = pl.ds(pl.multiple_of(core * rows + h * piece, piece), piece)
        return x_buf.at[q, at, pl.ds(pl.multiple_of(j * own, own), own)]

    tok_loads = []
    for h in range(2):
        source = tok_hbm.at[pl.ds(h * piece, piece)]
        tok_loads.append(pltpu.make_async_copy(source, unit(z, c, d, h), i_sem.at[2 + h]))
    ids_load = pltpu.make_async_copy(ids_hbm, ids, i_sem.at[0])
    levels_load = pltpu.make_async_copy(levels_hbm, levels, i_sem.at[1])
    for load in (*tok_loads, ids_load, levels_load):
        load.start()
    loads = {}
    for x in range(exp_dev):
        for i, (source, held) in enumerate(((gate_hbm, gate_w), (up_hbm, up_w))):
            loads[i, x] = pltpu.make_async_copy(source.at[x], held.at[x], w_sem.at[x, i])
    for x in range(exp_dev):
        loads[2, x] = pltpu.make_async_copy(down_hbm.at[x], down_w.at[x], w_sem.at[x, 2])
    for load in tok_loads:
        load.wait()
    for load in loads.values():
        load.start()
    pending = set(loads)

    def loaded(*keys):
        for key in keys:
            if key in pending:
                pending.remove(key)
                loads[key].wait()

    pl.semaphore_wait(barrier, 2 + jnp.minimum(z, 1) + jnp.minimum(chips - 1 - z, 1))

    shares = pl.ds(depth, 128)

    def swap(h):
        return pltpu.make_async_remote_copy(
            src_ref=unit(z, c, d, h), dst_ref=unit(z, c, d, h),
            send_sem=n_send, recv_sem=x_recv.at[z, d, h],
            device_id={"dp": 1 - d}, device_id_type=MESH,
        )

    def push(ref, q, way, sem):
        return pltpu.make_async_remote_copy(
            src_ref=ref, dst_ref=ref, send_sem=x_send.at[q, way], recv_sem=m_recv.at[q] if way == 0 else sem,
            device_id={"expert": (mate, e + 2, e - 2)[way]}, device_id_type=MESH,
        )

    def forward(q, j, h, way):
        return push(unit(q, c, j, h), q, way, x_recv.at[q, j, h])

    def forward_share(q, way):
        return push(x_buf.at[q, block(c), shares], q, way, c_recv.at[q])

    def await_copy(ref, sem, sent=False):
        copy = pltpu.make_async_remote_copy(
            src_ref=ref, dst_ref=ref, send_sem=sem if sent else t_send, recv_sem=t_send if sent else sem,
            device_id={"expert": mate}, device_id_type=MESH,
        )
        copy.wait_send() if sent else copy.wait_recv()

    def arrived(q, j, h):
        await_copy(unit(q, c, j, h), x_recv.at[q, j, h])

    def send_all(make):
        pl.when(z < chips - 1)(lambda: make(1).start())
        pl.when(z > 0)(lambda: make(2).start())
        make(0).start()

    def send_own(j, h):
        send_all(lambda way: forward(z, j, h, way))

    def pass_on(step, make, wait):
        for way in (1, 2):
            q = z - step if way == 1 else z + step
            inside = z >= step if way == 1 else z + step < chips
            further = jnp.logical_and(inside, z < chips - 1) if way == 1 else jnp.logical_and(inside, z > 0)

            @pl.when(inside)
            def _(q=q):
                wait(q)
                make(q, 0).start()

            @pl.when(further)
            def _(q=q, way=way):
                make(q, way).start()

    def relay(step, j, h):
        pass_on(step, lambda q, way: forward(q, j, h, way), lambda q: arrived(q, j, h))

    def relay_share(step):
        pass_on(step, forward_share, lambda q: await_copy(x_buf.at[q, block(c), shares], c_recv.at[q]))

    for h in range(2):
        swap(h).start()
    for h in range(2):
        send_own(d, h)
    ids_load.wait()
    levels_load.wait()
    label = lax.broadcasted_iota(jnp.int32, (128, rows), 0)
    share = jnp.zeros((128, rows), jnp.float32)
    for k in range(ids.shape[0]):
        level = levels[k : k + 1, :].astype(jnp.float32) / 256.0
        share = share + jnp.where(ids[k : k + 1, :] == label, level, 0.0)
    x_buf[z, block(c), shares] = share.T.astype(x_buf.dtype)
    send_all(lambda way: forward_share(z, way))

    table = visit_order(chips)
    order = []
    for step in range(chips):
        q = jnp.int32(0)
        for place in range(chips):
            q = jnp.where(z == place, jnp.int32(table[place][step]), q)
        order.append(q)

    def row_range(kind, start, size):
        if kind == "all":
            return pl.ds(start, size)
        core = c if kind == "own" else 1 - c
        return pl.ds(pl.multiple_of(core * rows + start, piece), size)

    items = crossings(chips, exp_dev, rows)
    spot = {item: i for i, item in enumerate(items)}

    def piece_of(i, side, t):
        role, kind, start, size, x = items[i]
        cols = pl.ds(pl.multiple_of(side * ff + t * WIDE, WIDE), WIDE)
        return hid.at[role, x, row_range(kind, start, size), cols]

    def cross(i, t):
        return pltpu.make_async_remote_copy(
            src_ref=piece_of(i, d, t), dst_ref=piece_of(i, d, t),
            send_sem=h_send, recv_sem=h_recv.at[i],
            device_id={"dp": 1 - d}, device_id_type=MESH,
        )

    def crossed(i):
        role, kind, start, size, x = items[i]
        cols = pl.ds(pl.multiple_of((1 - d) * ff, WIDE), ff)
        await_copy(hid.at[role, x, row_range(kind, start, size), cols], h_recv.at[i])

    seen = set()
    met = set()


    def enter(role, kind, x):
        if kind != "own" and role not in seen:
            seen.add(role)
            await_copy(x_buf.at[order[role], block(1 - c)], m_recv.at[order[role]])
        loaded((0, x), (1, x))

    def release(*chosen):
        for i in chosen:
            for t in range(ff // WIDE):
                cross(i, t).start()

    def units(role, kind, start, size, x, now=(), then=()):
        enter(role, kind, x)
        at = row_range(kind, start, size)

        def finish(t, gate, up):
            put = pl.ds(pl.multiple_of(d * ff + t * WIDE, WIDE), WIDE)
            hid[role, x, at, put] = (gate / (1.0 + jnp.exp(-gate)) * up).astype(hid.dtype)
            for i in now:
                cross(i, t).start()

        held = None
        for t in range(ff // WIDE):
            cols = slice(t * WIDE, (t + 1) * WIDE)
            lhs = x_buf[order[role], at, :depth]
            gate = jnp.dot(lhs, gate_w[x, :, cols], preferred_element_type=jnp.float32)
            up = jnp.dot(lhs, up_w[x, :, cols], preferred_element_type=jnp.float32)
            if held is not None:
                finish(*held)
            held = (t, gate, up)
        finish(*held)
        release(*then)

    def hand_over(role, t):
        return pltpu.make_async_remote_copy(
            src_ref=pair_out.at[role, t], dst_ref=pair_in.at[role, t],
            send_sem=p_send, recv_sem=p_recv.at[role, t],
            device_id={"expert": mate}, device_id_type=MESH,
        )

    def give_back(role, t):
        return pltpu.make_async_remote_copy(
            src_ref=ret_out.at[role, t], dst_ref=ret_in.at[z, t],
            send_sem=r_send, recv_sem=r_recv,
            device_id={"expert": order[role] * 2 + c}, device_id_type=MESH,
        )

    def share_of(role, at, size, x):
        lanes = lax.broadcasted_iota(jnp.int32, (size, 128), 1)
        picked = jnp.where(lanes == e * exp_dev + x, x_buf[order[role], at, shares].astype(jnp.float32), 0.0)
        return jnp.sum(picked, axis=1, keepdims=True)

    def outputs(role, kind, start, size, x, side=None, first=False, last=False, turn=None):
        at = row_range(kind, start, size)
        loaded((2, x))
        weight = share_of(role, at, size, x)
        if side != "own":
            for i, (a, b, begin, count, y) in enumerate(items):
                if (a, b, y) == (role, kind, x) and begin < start + size and start < begin + count and i not in met:
                    met.add(i)
                    crossed(i)
        if side is None:
            depth_at = slice(0, 2 * ff)
        else:
            depth_at = pl.ds(pl.multiple_of((d if side == "own" else 1 - d) * ff, WIDE), ff)

        def put(t, res):
            cols = slice(t * WIDE, (t + 1) * WIDE)
            res = res * weight
            if not first:
                res = res + acc[role, at, cols]
            if not last:
                acc[role, at, cols] = res
                return
            if kind == "mate":
                pair_out[role, t] = res.astype(pair_out.dtype)
                hand_over(role, t).start()
            elif turn is None:
                acc[role, at, cols] = res
                pair_out[role, t] = acc[role, block(1 - c), cols].astype(pair_out.dtype)
                hand_over(role, t).start()
            else:
                acc[role, at, cols] = res
                slot = jnp.where(c == turn, chips, role)
                pair_out[slot, t] = res.astype(pair_out.dtype)

                @pl.when(c != turn)
                def _():
                    hand_over(role, t).start()

        held = None
        for t in range(tiles):
            cols = slice(t * WIDE, (t + 1) * WIDE)
            res = jnp.dot(hid[role, x, at, depth_at], down_w[x, depth_at, cols], preferred_element_type=jnp.float32)
            if held is not None:
                put(*held)
            held = (t, res)
        put(*held)

    def combine(role, turn=None):
        def go():
            for t in range(tiles):
                cols = slice(t * WIDE, (t + 1) * WIDE)
                hand_over(role, t).wait_recv()
                both = acc[role, block(c), cols] + pair_in[role, t].astype(jnp.float32)
                ret_out[role, t] = both.astype(ret_out.dtype)
                give_back(role, t).start()

        go() if turn is None else pl.when(c == turn)(go)

    late = exp_dev - 1
    far = chips - 1

    def remote(role, x):
        if role == 1 and x < late:
            units(role, "all", 0, 2 * rows, x, now=(spot[role, "all", 0, 2 * rows, x],))
            return
        then = (spot[role, "all", rows, rows, y] for y in range(exp_dev)) if role > 1 and x == late else ()
        units(role, "all", 0, 2 * rows, x, now=(spot[role, "all", 0, rows, x],), then=then)

    def half(role, turn, side=None):
        for x in range(exp_dev):
            first = x == 0 and side is None
            outputs(role, "all", turn * rows, rows, x, side=side, first=first, last=x == late, turn=turn)

    arrived(z, 1 - d, 0)
    send_own(1 - d, 0)
    units(0, "own", 0, piece, 0, now=(0,))
    arrived(z, 1 - d, 1)
    send_own(1 - d, 1)
    units(0, "own", piece, piece, 0, now=(1,))
    units(0, "own", 0, rows, late, now=(2,))
    relay(1, d, 0)
    relay(1, d, 1)
    relay_share(1)
    relay(1, 1 - d, 0)
    units(0, "mate", 0, rows, 0, now=(3,))
    relay(1, 1 - d, 1)
    for x in range(1, late):
        units(0, "own", 0, rows, x)

    for step in range(1, chips):
        more = step + 1 < chips
        for x in range(late):
            remote(step, x)
        if step > 1:
            remote(step, late)
        if more:
            relay(step + 1, d, 0)
        if step == 1:
            remote(step, late)
        if more:
            relay(step + 1, d, 1)
            relay_share(step + 1)
        if step == 1:
            outputs(0, "own", 0, rows, 0, first=True)
        if more:
            relay(step + 1, 1 - d, 0)
        if step == 1:
            outputs(0, "mate", 0, rows, 0, first=True)
        if more:
            relay(step + 1, 1 - d, 1)
        if step > 3:
            for turn in range(2):
                half(step - 2, turn)
            for turn in range(2):
                combine(step - 2, turn)
    release(spot[1, "all", rows, rows, late])
    for x in range(1, exp_dev):
        units(0, "mate", 0, rows, x, now=(spot[0, "mate", 0, rows, x],))
    release(*(spot[0, "own", 0, rows, x] for x in range(1, late)), spot[0, "own", piece, piece, late])
    for x in range(late):
        outputs(1, "all", 0, 2 * rows, x, first=x == 0)
    outputs(1, "all", 0, rows, late, last=True, turn=0)
    if far > 2:
        half(far - 1, 0)
    combine(1, 0)
    if far > 2:
        half(far - 1, 1)
        combine(far - 1, 0)
    for x in range(exp_dev):
        outputs(far, "all", 0, 2 * rows, x, side="own", first=x == 0)
    if far > 2:
        combine(far - 1, 1)
    outputs(1, "all", rows, rows, late, side="own")
    for x in range(1, exp_dev):
        outputs(0, "mate", 0, rows, x, side="own")
        outputs(0, "own", 0, rows, x, side="own")
    half(far, 0, side="other")
    for x in range(late):
        outputs(far, "all", rows, rows, x, side="other")
    combine(far, 0)
    outputs(far, "all", rows, rows, late, side="other", last=True, turn=1)
    combine(far, 1)
    outputs(1, "all", rows, rows, late, side="other", last=True, turn=1)
    for x in range(1, late):
        outputs(0, "mate", 0, rows, x, side="other")
    combine(1, 1)
    outputs(0, "mate", 0, rows, late, side="other", last=True)
    for x in range(1, exp_dev):
        outputs(0, "own", 0, rows, x, side="other")

    for t in range(tiles):
        hand_over(0, t).wait_recv()
    await_copy(ret_in.at[pl.ds(0, chips - 1)], r_recv)
    for t in range(tiles):
        cols = slice(t * WIDE, (t + 1) * WIDE)
        full = acc[0, block(c), cols] + pair_in[0, t].astype(jnp.float32)
        for i in range(1, chips):
            full = full + ret_in[lax.rem(z + i, chips), t].astype(jnp.float32)
        out[:, cols] = full.astype(out.dtype)

    await_copy(x_buf.at[z, block(c), pl.ds(pl.multiple_of(d * own, own), own)], n_send, sent=True)
    for q in range(chips):
        await_copy(x_buf.at[q, block(c)], x_send.at[q, 0], sent=True)
        for way, sends in ((1, jnp.logical_and(q <= z, z < chips - 1)), (2, jnp.logical_and(q >= z, z > 0))):
            @pl.when(sends)
            def _(q=q, way=way):
                await_copy(x_buf.at[q, block(c)], x_send.at[q, way], sent=True)
    await_copy(hid.at[:, :, :, pl.ds(pl.multiple_of(d * ff, WIDE), ff)], h_send, sent=True)
    await_copy(pair_out.at[pl.ds(0, chips)], p_send, sent=True)
    await_copy(ret_out.at[pl.ds(1, chips - 1)], r_send, sent=True)


def dense_on_device(tokens, expert_ids, gate_levels, gate_weight, up_weight, down_weight):
    chips = lax.axis_size("expert") // 2
    rows, own = tokens.shape
    exp_dev, depth, ff = gate_weight.shape
    width = down_weight.shape[2]
    kind = tokens.dtype
    tiles = width // WIDE
    picks = expert_ids.shape[1]
    count = len(crossings(chips, exp_dev, rows))
    anywhere = pl.BlockSpec(memory_space=pl.ANY)
    dma = pltpu.SemaphoreType.DMA
    operands = [
        pltpu.with_memory_space_constraint(a, memory_space=pltpu.HBM)
        for a in (tokens, expert_ids.T, gate_levels.T, gate_weight, up_weight, down_weight)
    ]
    flops = 2 * chips * 2 * rows * exp_dev * (2 * depth * ff + 2 * ff * width)
    return pl.pallas_call(
        functools.partial(dense_kernel, chips),
        out_shape=jax.ShapeDtypeStruct((rows, width), kind),
        in_specs=[anywhere] * 6,
        out_specs=pl.BlockSpec(memory_space=pltpu.VMEM),
        scratch_shapes=[
            pltpu.VMEM((picks, rows), jnp.int32),
            pltpu.VMEM((picks, rows), jnp.int32),
            pltpu.VMEM(gate_weight.shape, kind),
            pltpu.VMEM(up_weight.shape, kind),
            pltpu.VMEM(down_weight.shape, kind),
            pltpu.VMEM((chips, 2 * rows, depth + 128), kind),
            pltpu.VMEM((chips, exp_dev, 2 * rows, 2 * ff), kind),
            pltpu.VMEM((chips, 2 * rows, width), jnp.float32),
            pltpu.VMEM((chips + 1, tiles, rows, WIDE), kind),
            pltpu.VMEM((chips, tiles, rows, WIDE), kind),
            pltpu.VMEM((chips, tiles, rows, WIDE), kind),
            pltpu.VMEM((chips, tiles, rows, WIDE), kind),
            dma((4,)),
            dma((exp_dev, 3)),
            dma((chips, 3)),
            dma((chips, 2, 2)),
            dma((chips,)),
            dma((chips,)),
            dma,
            dma,
            dma,
            dma((count,)),
            dma,
            dma((chips, tiles)),
            dma,
            dma,
        ],
        compiler_params=pltpu.CompilerParams(
            collective_id=0, has_side_effects=True, vmem_limit_bytes=50331648
        ),
        cost_estimate=pl.CostEstimate(
            flops=flops, bytes_accessed=2 * 3 * gate_weight.size, transcendentals=0
        ),
    )(*operands)


def on_device(tokens, expert_ids, gate_levels, gate_weight, up_weight, down_weight):
    rows, own = tokens.shape
    exp_dev, depth, ff = gate_weight.shape
    n_expert = lax.axis_size("expert")
    width = down_weight.shape[2]
    experts = exp_dev * n_expert
    dense = (
        2 * rows * expert_ids.shape[1] >= rows * experts
        and lax.axis_size("dp") == 2
        and n_expert % 2 == 0
        and n_expert >= 6
        and experts <= 128
        and rows % 32 == 0
        and exp_dev >= 2
        and own % 128 == 0
        and ff % WIDE == 0
        and width % WIDE == 0
    )
    call = dense_on_device if dense else routed_on_device
    return call(tokens, expert_ids, gate_levels, gate_weight, up_weight, down_weight)


def solution(mesh):
    in_specs = (
        P(("groups", "expert"), "dp"),
        P(("groups", "expert"), None),
        P(("groups", "expert"), None),
        P("expert", None, "dp"),
        P("expert", None, "dp"),
        P("expert", None, "dp"),
    )
    out_specs = P(("groups", "expert"), "dp")
    return jax.shard_map(
        on_device, mesh=mesh, in_specs=in_specs, out_specs=out_specs, check_vma=False
    )
```

```python
import functools

import jax
import jax.numpy as jnp
from jax import lax
from jax.experimental import pallas as pl
from jax.experimental.pallas import tpu as pltpu
from jax.sharding import PartitionSpec as P

MESH = pl.DeviceIdType.MESH
WIDE = 256


def slot_numbers(chosen_ids, experts, capacity):
    flat_ids = chosen_ids.reshape(-1)
    labels = jnp.arange(experts, dtype=jnp.int32)
    onehot = (flat_ids[:, None] == labels[None, :]).astype(jnp.int32)
    before = jnp.cumsum(onehot, axis=0) - onehot
    position = jnp.sum(before * onehot, axis=1)
    return (flat_ids * capacity + position).reshape(chosen_ids.shape)


def route_matrix(slots, count):
    targets = jnp.arange(count, dtype=jnp.int32)
    return jnp.any(targets[:, None, None] == slots[None, :, :], axis=2).astype(jnp.bfloat16)


def routed_on_device(tokens, expert_ids, gate_levels, gate_weight, up_weight, down_weight):
    tok_dev = tokens.shape[0]
    picks = expert_ids.shape[1]
    exp_dev = gate_weight.shape[0]
    n_expert = lax.axis_size("expert")
    experts = exp_dev * n_expert
    capacity = min(tok_dev, max(2, 2 * tok_dev * picks // experts))
    slot_count = experts * capacity
    own_slots = slot_numbers(expert_ids, experts, capacity)
    route = route_matrix(own_slots, slot_count)
    whole = lax.all_gather(tokens, "dp", axis=1, tiled=True)
    outgoing = jnp.dot(route, whole, preferred_element_type=jnp.float32).astype(jnp.bfloat16)
    outgoing = outgoing.reshape(n_expert, exp_dev, capacity, whole.shape[1])
    arrived = lax.all_to_all(outgoing, "expert", split_axis=0, concat_axis=0, tiled=True)
    gate_part = jnp.einsum(
        "sxcd,xdf->sxcf", arrived, gate_weight, preferred_element_type=jnp.float32
    )
    up_part = jnp.einsum("sxcd,xdf->sxcf", arrived, up_weight, preferred_element_type=jnp.float32)
    hidden = (jax.nn.silu(gate_part) * up_part).astype(jnp.bfloat16)
    out_features = down_weight.shape[2]
    outputs = jnp.einsum(
        "sxcf,xfk->sxck",
        lax.all_gather(hidden, "dp", axis=3, tiled=True),
        down_weight,
        preferred_element_type=jnp.float32,
    )
    result = outputs.astype(jnp.bfloat16)
    returned = lax.all_to_all(result, "expert", split_axis=0, concat_axis=0, tiled=True)
    returned = returned.reshape(slot_count, out_features)
    shares = gate_levels.astype(jnp.float32) / 256.0
    targets = jnp.arange(slot_count, dtype=jnp.int32)
    weighting = jnp.sum(
        jnp.where(
            targets[None, :, None] == own_slots[:, None, :], shares[:, None, :], jnp.float32(0.0)
        ),
        axis=2,
    )
    weighting = weighting.astype(jnp.bfloat16)
    combined = jnp.dot(weighting, returned, preferred_element_type=jnp.float32)
    return combined.astype(jnp.bfloat16)


def visit_order(chips):
    table = []
    for z in range(chips):
        up = 2 * z < chips
        inward = sorted((q for q in range(chips) if q != z and (q > z) == up), key=lambda q: abs(q - z))
        outward = sorted((q for q in range(chips) if q != z and (q > z) != up), key=lambda q: -abs(q - z))
        table.append([z, *inward, *outward])
    return table


def crossings(chips, exp_dev, rows):
    piece, late = rows // 2, exp_dev - 1
    parts = [(0, "own", 0, piece, 0), (0, "own", piece, piece, 0), (0, "own", 0, piece, late), (0, "mate", 0, rows, 0)]
    for x in range(late):
        parts += [(1, "own", 0, rows, x), (1, "mate", 0, rows, x)]
    for turn in range(2):
        parts.append((1, "all", turn * rows, rows, late))
    for role in range(2, chips):
        for turn in range(2):
            for x in range(exp_dev):
                parts.append((role, "all", turn * rows, rows, x))
    for x in range(1, exp_dev):
        parts.append((0, "mate", 0, rows, x))
    for x in range(1, late):
        parts.append((0, "own", 0, rows, x))
    parts.append((0, "own", piece, piece, late))
    return parts


def dense_kernel(
    chips, tok_hbm, ids_hbm, levels_hbm, gate_hbm, up_hbm, down_hbm, out,
    ids, levels, gate_w, up_w, down_w, x_buf, hid, acc, pair_out, pair_in, ret_out, ret_in,
    i_sem, w_sem, x_send, x_recv, c_recv, m_recv, t_send, n_send, h_send, h_recv, p_send, p_recv, r_send, r_recv,
):
    e = lax.axis_index("expert")
    d = lax.axis_index("dp")
    z, c = lax.div(e, 2), lax.rem(e, 2)
    rows, own = tok_hbm.shape
    exp_dev, depth, ff = gate_w.shape
    width = down_w.shape[2]
    tiles = width // WIDE
    piece = rows // 2
    mate = z * 2 + 1 - c

    barrier = pltpu.get_barrier_semaphore()
    pl.semaphore_signal(barrier, inc=1, device_id={"dp": 1 - d}, device_id_type=MESH)
    pl.semaphore_signal(barrier, inc=1, device_id={"expert": mate}, device_id_type=MESH)

    @pl.when(z > 0)
    def _():
        pl.semaphore_signal(barrier, inc=1, device_id={"expert": e - 2}, device_id_type=MESH)

    @pl.when(z < chips - 1)
    def _():
        pl.semaphore_signal(barrier, inc=1, device_id={"expert": e + 2}, device_id_type=MESH)

    def block(core):
        return pl.ds(pl.multiple_of(core * rows, rows), rows)

    def unit(q, core, j, h):
        at = pl.ds(pl.multiple_of(core * rows + h * piece, piece), piece)
        return x_buf.at[q, at, pl.ds(pl.multiple_of(j * own, own), own)]

    tok_loads = []
    for h in range(2):
        source = tok_hbm.at[pl.ds(h * piece, piece)]
        tok_loads.append(pltpu.make_async_copy(source, unit(z, c, d, h), i_sem.at[2 + h]))
    ids_load = pltpu.make_async_copy(ids_hbm, ids, i_sem.at[0])
    levels_load = pltpu.make_async_copy(levels_hbm, levels, i_sem.at[1])
    for load in (*tok_loads, ids_load, levels_load):
        load.start()
    loads = {}
    for x in range(exp_dev):
        for i, (source, held) in enumerate(((gate_hbm, gate_w), (up_hbm, up_w))):
            loads[i, x] = pltpu.make_async_copy(source.at[x], held.at[x], w_sem.at[x, i])
    for x in range(exp_dev):
        loads[2, x] = pltpu.make_async_copy(down_hbm.at[x], down_w.at[x], w_sem.at[x, 2])
    for load in tok_loads:
        load.wait()
    for load in loads.values():
        load.start()
    pending = set(loads)

    def loaded(*keys):
        for key in keys:
            if key in pending:
                pending.remove(key)
                loads[key].wait()

    pl.semaphore_wait(barrier, 2 + jnp.minimum(z, 1) + jnp.minimum(chips - 1 - z, 1))

    shares = pl.ds(depth, 128)

    def swap(h):
        return pltpu.make_async_remote_copy(
            src_ref=unit(z, c, d, h), dst_ref=unit(z, c, d, h),
            send_sem=n_send, recv_sem=x_recv.at[z, d, h],
            device_id={"dp": 1 - d}, device_id_type=MESH,
        )

    def push(ref, q, way, sem):
        return pltpu.make_async_remote_copy(
            src_ref=ref, dst_ref=ref, send_sem=x_send.at[way], recv_sem=m_recv.at[q] if way == 0 else sem,
            device_id={"expert": (mate, e + 2, e - 2)[way]}, device_id_type=MESH,
        )

    def forward(q, j, h, way):
        return push(unit(q, c, j, h), q, way, x_recv.at[q, j, h])

    def forward_share(q, way):
        return push(x_buf.at[q, block(c), shares], q, way, c_recv.at[q])

    def await_copy(ref, sem, sent=False):
        copy = pltpu.make_async_remote_copy(
            src_ref=ref, dst_ref=ref, send_sem=sem if sent else t_send, recv_sem=t_send if sent else sem,
            device_id={"expert": mate}, device_id_type=MESH,
        )
        copy.wait_send() if sent else copy.wait_recv()

    def arrived(q, j, h):
        await_copy(unit(q, c, j, h), x_recv.at[q, j, h])

    def send_all(make):
        pl.when(z < chips - 1)(lambda: make(1).start())
        pl.when(z > 0)(lambda: make(2).start())
        make(0).start()

    def send_own(j, h):
        send_all(lambda way: forward(z, j, h, way))

    def pass_on(step, make, wait):
        for way in (1, 2):
            q = z - step if way == 1 else z + step
            inside = z >= step if way == 1 else z + step < chips
            further = jnp.logical_and(inside, z < chips - 1) if way == 1 else jnp.logical_and(inside, z > 0)

            @pl.when(inside)
            def _(q=q):
                wait(q)
                make(q, 0).start()

            @pl.when(further)
            def _(q=q, way=way):
                make(q, way).start()

    def relay(step, j, h):
        pass_on(step, lambda q, way: forward(q, j, h, way), lambda q: arrived(q, j, h))

    def relay_share(step):
        pass_on(step, forward_share, lambda q: await_copy(x_buf.at[q, block(c), shares], c_recv.at[q]))

    for h in range(2):
        swap(h).start()
    for h in range(2):
        send_own(d, h)
    ids_load.wait()
    levels_load.wait()
    label = lax.broadcasted_iota(jnp.int32, (128, rows), 0)
    share = jnp.zeros((128, rows), jnp.float32)
    for k in range(ids.shape[0]):
        level = levels[k : k + 1, :].astype(jnp.float32) / 256.0
        share = share + jnp.where(ids[k : k + 1, :] == label, level, 0.0)
    x_buf[z, block(c), shares] = share.T.astype(x_buf.dtype)
    send_all(lambda way: forward_share(z, way))

    table = visit_order(chips)
    order = []
    for step in range(chips):
        q = jnp.int32(0)
        for place in range(chips):
            q = jnp.where(z == place, jnp.int32(table[place][step]), q)
        order.append(q)

    def row_range(kind, start, size):
        if kind == "all":
            return pl.ds(start, size)
        core = c if kind == "own" else 1 - c
        return pl.ds(pl.multiple_of(core * rows + start, piece), size)

    items = crossings(chips, exp_dev, rows)
    spot = {item: i for i, item in enumerate(items)}

    def piece_of(i, side, t):
        role, kind, start, size, x = items[i]
        cols = pl.ds(pl.multiple_of(side * ff + t * WIDE, WIDE), WIDE)
        return hid.at[role, x, row_range(kind, start, size), cols]

    def cross(i, t):
        return pltpu.make_async_remote_copy(
            src_ref=piece_of(i, d, t), dst_ref=piece_of(i, d, t),
            send_sem=h_send, recv_sem=h_recv.at[i],
            device_id={"dp": 1 - d}, device_id_type=MESH,
        )

    def crossed(i):
        role, kind, start, size, x = items[i]
        cols = pl.ds(pl.multiple_of((1 - d) * ff, WIDE), ff)
        await_copy(hid.at[role, x, row_range(kind, start, size), cols], h_recv.at[i])

    seen = set()
    met = set()


    def enter(role, kind, x):
        if kind != "own" and role not in seen:
            seen.add(role)
            await_copy(x_buf.at[order[role], block(1 - c)], m_recv.at[order[role]])
        loaded((0, x), (1, x))

    def release(*chosen):
        for i in chosen:
            for t in range(ff // WIDE):
                cross(i, t).start()

    def units(role, kind, start, size, x, now=(), then=()):
        enter(role, kind, x)
        at = row_range(kind, start, size)

        def finish(t, gate, up):
            put = pl.ds(pl.multiple_of(d * ff + t * WIDE, WIDE), WIDE)
            hid[role, x, at, put] = (gate / (1.0 + jnp.exp(-gate)) * up).astype(hid.dtype)
            for i in now:
                cross(i, t).start()

        held = None
        for t in range(ff // WIDE):
            cols = slice(t * WIDE, (t + 1) * WIDE)
            lhs = x_buf[order[role], at, :depth]
            gate = jnp.dot(lhs, gate_w[x, :, cols], preferred_element_type=jnp.float32)
            up = jnp.dot(lhs, up_w[x, :, cols], preferred_element_type=jnp.float32)
            if held is not None:
                finish(*held)
            held = (t, gate, up)
        finish(*held)
        release(*then)

    def hand_over(role, t):
        return pltpu.make_async_remote_copy(
            src_ref=pair_out.at[role, t], dst_ref=pair_in.at[role, t],
            send_sem=p_send, recv_sem=p_recv.at[role, t],
            device_id={"expert": mate}, device_id_type=MESH,
        )

    def give_back(role, t):
        return pltpu.make_async_remote_copy(
            src_ref=ret_out.at[role, t], dst_ref=ret_in.at[z, t],
            send_sem=r_send, recv_sem=r_recv,
            device_id={"expert": order[role] * 2 + c}, device_id_type=MESH,
        )

    def share_of(role, at, size, x):
        lanes = lax.broadcasted_iota(jnp.int32, (size, 128), 1)
        picked = jnp.where(lanes == e * exp_dev + x, x_buf[order[role], at, shares].astype(jnp.float32), 0.0)
        return jnp.sum(picked, axis=1, keepdims=True)

    def outputs(role, kind, start, size, x, side=None, first=False, last=False, turn=None):
        at = row_range(kind, start, size)
        loaded((2, x))
        weight = share_of(role, at, size, x)
        if side != "own":
            for i, (a, b, begin, count, y) in enumerate(items):
                same = b == kind and begin < start + size and start < begin + count
                if (a, y) == (role, x) and (same or (kind == "all" and b != "all")) and i not in met:
                    met.add(i)
                    crossed(i)
        if side is None:
            depth_at = slice(0, 2 * ff)
        else:
            depth_at = pl.ds(pl.multiple_of((d if side == "own" else 1 - d) * ff, WIDE), ff)

        def put(t, res):
            cols = slice(t * WIDE, (t + 1) * WIDE)
            res = res * weight
            if not first:
                res = res + acc[role, at, cols]
            if not last:
                acc[role, at, cols] = res
                return
            if kind == "mate":
                pair_out[role, t] = res.astype(pair_out.dtype)
                hand_over(role, t).start()
            elif turn is None:
                acc[role, at, cols] = res
                pair_out[role, t] = acc[role, block(1 - c), cols].astype(pair_out.dtype)
                hand_over(role, t).start()
            else:
                acc[role, at, cols] = res
                slot = jnp.where(c == turn, chips, role)
                pair_out[slot, t] = res.astype(pair_out.dtype)

                @pl.when(c != turn)
                def _():
                    hand_over(role, t).start()

        held = None
        for t in range(tiles):
            cols = slice(t * WIDE, (t + 1) * WIDE)
            res = jnp.dot(hid[role, x, at, depth_at], down_w[x, depth_at, cols], preferred_element_type=jnp.float32)
            if held is not None:
                put(*held)
            held = (t, res)
        put(*held)

    def combine(role, turn=None):
        def go():
            for t in range(tiles):
                cols = slice(t * WIDE, (t + 1) * WIDE)
                hand_over(role, t).wait_recv()
                both = acc[role, block(c), cols] + pair_in[role, t].astype(jnp.float32)
                ret_out[role, t] = both.astype(ret_out.dtype)
                give_back(role, t).start()

        go() if turn is None else pl.when(c == turn)(go)

    late = exp_dev - 1
    far = chips - 1

    def remote(role, x):
        if role == 1 and x < late:
            for kind in ("own", "mate"):
                units(role, kind, 0, rows, x, now=(spot[role, kind, 0, rows, x],))
            return
        then = ()
        if 1 < role < far:
            then = (spot[role, "all", rows, rows, x],)
        elif role == far and x == late:
            then = (spot[role, "all", rows, rows, y] for y in range(exp_dev))
        units(role, "all", 0, 2 * rows, x, now=(spot[role, "all", 0, rows, x],), then=then)

    def half(role, turn, side=None):
        for x in range(exp_dev):
            first = x == 0 and side is None
            outputs(role, "all", turn * rows, rows, x, side=side, first=first, last=x == late, turn=turn)

    arrived(z, 1 - d, 0)
    send_own(1 - d, 0)
    units(0, "own", 0, piece, 0, now=(0,))
    arrived(z, 1 - d, 1)
    send_own(1 - d, 1)
    units(0, "own", piece, piece, 0, now=(1,))
    units(0, "own", 0, rows, late, now=(2,))
    relay(1, d, 0)
    relay(1, d, 1)
    relay_share(1)
    relay(1, 1 - d, 0)
    units(0, "mate", 0, rows, 0, now=(3,))
    relay(1, 1 - d, 1)
    for x in range(1, late):
        units(0, "own", 0, rows, x)

    for step in range(1, chips):
        more = step + 1 < chips
        for x in range(late):
            remote(step, x)
        if step > 1:
            remote(step, late)
        if more:
            relay(step + 1, d, 0)
        if step == 1:
            remote(step, late)
        if more:
            relay(step + 1, d, 1)
            relay_share(step + 1)
        if step == 1:
            outputs(0, "own", 0, rows, 0, first=True)
        if more:
            relay(step + 1, 1 - d, 0)
        if step == 1:
            outputs(0, "mate", 0, rows, 0, first=True)
        if more:
            relay(step + 1, 1 - d, 1)
        if step > 3:
            for turn in range(2):
                half(step - 2, turn)
            for turn in range(2):
                combine(step - 2, turn)
    release(spot[1, "all", rows, rows, late])
    for x in range(1, exp_dev):
        units(0, "mate", 0, rows, x, now=(spot[0, "mate", 0, rows, x],))
    release(*(spot[0, "own", 0, rows, x] for x in range(1, late)), spot[0, "own", piece, piece, late])
    for x in range(late):
        outputs(1, "all", 0, 2 * rows, x, first=x == 0)
    outputs(1, "all", 0, rows, late, last=True, turn=0)
    if far > 2:
        half(far - 1, 0)
    combine(1, 0)
    if far > 2:
        half(far - 1, 1)
        combine(far - 1, 0)
    for x in range(exp_dev):
        outputs(far, "all", 0, 2 * rows, x, side="own", first=x == 0)
    if far > 2:
        combine(far - 1, 1)
    outputs(1, "all", rows, rows, late, side="own")
    for x in range(1, exp_dev):
        outputs(0, "mate", 0, rows, x, side="own")
        outputs(0, "own", 0, rows, x, side="own")
    half(far, 0, side="other")
    for x in range(late):
        outputs(far, "all", rows, rows, x, side="other")
    combine(far, 0)
    outputs(far, "all", rows, rows, late, side="other", last=True, turn=1)
    combine(far, 1)
    outputs(1, "all", rows, rows, late, side="other", last=True, turn=1)
    for x in range(1, late):
        outputs(0, "mate", 0, rows, x, side="other")
    combine(1, 1)
    outputs(0, "mate", 0, rows, late, side="other", last=True)
    for x in range(1, exp_dev):
        outputs(0, "own", 0, rows, x, side="other")

    for t in range(tiles):
        hand_over(0, t).wait_recv()
    await_copy(ret_in.at[pl.ds(0, chips - 1)], r_recv)
    for t in range(tiles):
        cols = slice(t * WIDE, (t + 1) * WIDE)
        full = acc[0, block(c), cols] + pair_in[0, t].astype(jnp.float32)
        for i in range(1, chips):
            full = full + ret_in[lax.rem(z + i, chips), t].astype(jnp.float32)
        out[:, cols] = full.astype(out.dtype)

    await_copy(x_buf.at[z, block(c), pl.ds(pl.multiple_of(d * own, own), own)], n_send, sent=True)
    await_copy(x_buf.at[:, block(c)], x_send.at[0], sent=True)
    for place in range(chips):
        @pl.when(z == place)
        def _(place=place):
            if place < chips - 1:
                await_copy(x_buf.at[pl.ds(0, place + 1), block(c)], x_send.at[1], sent=True)
            if place > 0:
                await_copy(x_buf.at[pl.ds(place, chips - place), block(c)], x_send.at[2], sent=True)

    await_copy(hid.at[:, :, :, pl.ds(pl.multiple_of(d * ff, WIDE), ff)], h_send, sent=True)
    await_copy(pair_out.at[pl.ds(0, chips)], p_send, sent=True)
    await_copy(ret_out.at[pl.ds(1, chips - 1)], r_send, sent=True)


def dense_on_device(tokens, expert_ids, gate_levels, gate_weight, up_weight, down_weight):
    chips = lax.axis_size("expert") // 2
    rows, own = tokens.shape
    exp_dev, depth, ff = gate_weight.shape
    width = down_weight.shape[2]
    kind = tokens.dtype
    tiles = width // WIDE
    picks = expert_ids.shape[1]
    count = len(crossings(chips, exp_dev, rows))
    anywhere = pl.BlockSpec(memory_space=pl.ANY)
    dma = pltpu.SemaphoreType.DMA
    operands = [
        pltpu.with_memory_space_constraint(a, memory_space=pltpu.HBM)
        for a in (tokens, expert_ids.T, gate_levels.T, gate_weight, up_weight, down_weight)
    ]
    flops = 2 * chips * 2 * rows * exp_dev * (2 * depth * ff + 2 * ff * width)
    return pl.pallas_call(
        functools.partial(dense_kernel, chips),
        out_shape=jax.ShapeDtypeStruct((rows, width), kind),
        in_specs=[anywhere] * 6,
        out_specs=pl.BlockSpec(memory_space=pltpu.VMEM),
        scratch_shapes=[
            pltpu.VMEM((picks, rows), jnp.int32),
            pltpu.VMEM((picks, rows), jnp.int32),
            pltpu.VMEM(gate_weight.shape, kind),
            pltpu.VMEM(up_weight.shape, kind),
            pltpu.VMEM(down_weight.shape, kind),
            pltpu.VMEM((chips, 2 * rows, depth + 128), kind),
            pltpu.VMEM((chips, exp_dev, 2 * rows, 2 * ff), kind),
            pltpu.VMEM((chips, 2 * rows, width), jnp.float32),
            pltpu.VMEM((chips + 1, tiles, rows, WIDE), kind),
            pltpu.VMEM((chips, tiles, rows, WIDE), kind),
            pltpu.VMEM((chips, tiles, rows, WIDE), kind),
            pltpu.VMEM((chips, tiles, rows, WIDE), kind),
            dma((4,)),
            dma((exp_dev, 3)),
            dma((3,)),
            dma((chips, 2, 2)),
            dma((chips,)),
            dma((chips,)),
            dma,
            dma,
            dma,
            dma((count,)),
            dma,
            dma((chips, tiles)),
            dma,
            dma,
        ],
        compiler_params=pltpu.CompilerParams(
            collective_id=0, has_side_effects=True, vmem_limit_bytes=50331648
        ),
        cost_estimate=pl.CostEstimate(
            flops=flops, bytes_accessed=2 * 3 * gate_weight.size, transcendentals=0
        ),
    )(*operands)


def on_device(tokens, expert_ids, gate_levels, gate_weight, up_weight, down_weight):
    rows, own = tokens.shape
    exp_dev, depth, ff = gate_weight.shape
    n_expert = lax.axis_size("expert")
    width = down_weight.shape[2]
    experts = exp_dev * n_expert
    dense = (
        2 * rows * expert_ids.shape[1] >= rows * experts
        and lax.axis_size("dp") == 2
        and n_expert % 2 == 0
        and n_expert >= 6
        and experts <= 128
        and rows % 32 == 0
        and exp_dev >= 2
        and own % 128 == 0
        and ff % WIDE == 0
        and width % WIDE == 0
    )
    call = dense_on_device if dense else routed_on_device
    return call(tokens, expert_ids, gate_levels, gate_weight, up_weight, down_weight)


def solution(mesh):
    in_specs = (
        P(("groups", "expert"), "dp"),
        P(("groups", "expert"), None),
        P(("groups", "expert"), None),
        P("expert", None, "dp"),
        P("expert", None, "dp"),
        P("expert", None, "dp"),
    )
    out_specs = P(("groups", "expert"), "dp")
    return jax.shard_map(
        on_device, mesh=mesh, in_specs=in_specs, out_specs=out_specs, check_vma=False
    )
```
